16 devices in a mesh: dp: 1, tp: 16 (over x, y, z, core).
Axes of the slice: x: 2, y: 2, z: 2, core: 2. Of those that a mesh axis runs over, the one named last changes fastest.
Arguments:
- x: bfloat16 [2048, 12288], P('dp')
- w_gate: bfloat16 [12288, 28672], P(None, 'tp')
- w_up: bfloat16 [12288, 28672], P(None, 'tp')
- w_down: bfloat16 [28672, 12288], P('tp')
Outputs:
- output: bfloat16 [2048, 12288], P('dp')
All inputs are finite; a program needn't handle non-finite values.
Results may differ from the reference program's by a relative error of at most 0.016.
Values are sent between devices in bfloat16 or wider.
A program may use at most 2 GiB of HBM per device.

```python
import jax
import jax.numpy as jnp

ROWS = 2048
D = 12288
FF = 28672


def setup_inputs(seed: int = 0, part: int = 0) -> dict:
    kx, kg, ku, kd = jax.random.split(jax.random.key(seed), 4)
    drawn = {
        "x": jax.random.normal(jax.random.fold_in(kx, part), (ROWS, D), jnp.float32),
        "w_gate": jax.random.normal(kg, (D, FF), jnp.float32) * D**-0.5,
        "w_up": jax.random.normal(ku, (D, FF), jnp.float32) * D**-0.5,
        "w_down": jax.random.normal(kd, (FF, D), jnp.float32) * FF**-0.5,
    }
    return {k: v.astype(jnp.bfloat16) for k, v in drawn.items()}


def reference(x, w_gate, w_up, w_down):
    gate = jnp.dot(x, w_gate, preferred_element_type=jnp.float32)
    up = jnp.dot(x, w_up, preferred_element_type=jnp.float32)
    hidden = (jax.nn.silu(gate) * up).astype(jnp.bfloat16)
    return jnp.dot(hidden, w_down, preferred_element_type=jnp.float32).astype(jnp.bfloat16)
```

```python
import functools

import jax
import jax.numpy as jnp
from jax import lax
from jax.experimental import pallas as pl
from jax.experimental.pallas import tpu as pltpu
from jax.sharding import PartitionSpec as P

MESH = pl.DeviceIdType.MESH
F32, BF16 = jnp.float32, jnp.bfloat16

R = 512
HALF = R // 2
CB = 512
KB = 6144
GN = 256
WD_STEPS = 27


def kernel(x_hbm, wg_hbm, wu_hbm, wd_hbm, y_hbm,
           xv, wbuf, acc, hv, dbuf, rv0, rv1, rv2, rv3, st0, st1, st2, st3, stf,
           x_sem, w_sem, d_sem, s0s, s1s, s2s, s3s, fs, fl, a3s, a2s, a1s,
           r0, r1, r2, r3, g3, g2, g1, g0, credit):
    rows, depth = x_hbm.shape
    units = wg_hbm.shape[1]
    nc = rows // R
    nt = units // GN
    me = lax.axis_index("tp")
    b0 = lax.rem(me, 2)

    def dim(k, s):
        return lax.rem(k + s, 3)

    def mask(d):
        return jnp.where(d == 0, 8, jnp.where(d == 1, 4, 2))

    def bit(d):
        return lax.rem(me // mask(d), 2)

    def peer(d):
        m = mask(d)
        return me + m - 2 * m * bit(d)

    core_peer = me + 1 - 2 * b0

    def bits(k):
        return bit(dim(k, 0)), bit(dim(k, 1)), bit(dim(k, 2))

    def col(k, i0, i1, i2):
        return pl.multiple_of((k * 8 + i0 * 4 + i1 * 2 + i2) * CB, CB)

    def to(dev):
        return dict(device_id={"tp": dev}, device_id_type=MESH)

    barrier = pltpu.get_barrier_semaphore()
    everyone = [peer(0), peer(1), peer(2), core_peer]
    for dev in everyone:
        pl.semaphore_signal(barrier, inc=1, **to(dev))
    pl.semaphore_wait(barrier, 4)

    def w_copies(q):
        n, kk, slot = lax.rem(q // 2, nt), lax.rem(q, 2), lax.rem(q, 2)
        src = (pl.ds(pl.multiple_of(kk * KB, KB), KB), pl.ds(pl.multiple_of(n * GN, GN), GN))
        return [
            pltpu.make_async_copy(wg_hbm.at[src], wbuf.at[slot, :, pl.ds(0, GN)], w_sem.at[slot, 0]),
            pltpu.make_async_copy(wu_hbm.at[src], wbuf.at[slot, :, pl.ds(GN, GN)], w_sem.at[slot, 1]),
        ]

    def w_start(q):
        @pl.when(q < nc * nt * 2)
        def _():
            for c in w_copies(q):
                c.start()

    def wd_col(step):
        r = lax.rem(step, WD_STEPS)
        early = r < 18
        group = r // 6
        k = jnp.where(early, lax.rem(r, 6) // 2, lax.rem(r, 3))
        j = lax.rem(r, 2)
        s1, s2, _ = bits(k)
        i0 = jnp.where(early & (group != 1), 1 - b0, b0)
        i1 = jnp.where(early & (group != 2), 1 - s1, s1)
        flip = (early & (j == 0)) | (r // 3 == 6)
        i2 = jnp.where(flip, 1 - s2, s2)
        return col(k, i0, i1, i2)

    def d_copy(step):
        slot = lax.rem(step, 3)
        return pltpu.make_async_copy(wd_hbm.at[:, pl.ds(wd_col(step), CB)], dbuf.at[slot], d_sem.at[slot])

    def d_start(step):
        @pl.when(step < nc * WD_STEPS)
        def _():
            d_copy(step).start()

    def d_next(step):
        d_copy(step).wait()
        d_start(step + 2)
        return lax.rem(step, 3)

    def x_copies(c):
        return [
            pltpu.make_async_copy(
                x_hbm.at[pl.ds(pl.multiple_of(c * R, R), R), pl.ds(i * KB, KB)], xv.at[i], x_sem.at[i]
            )
            for i in range(2)
        ]

    for c in x_copies(0):
        c.start()
    w_start(0)
    w_start(1)
    d_start(0)
    d_start(1)

    def gate_up(c, n):
        q = (c * nt + n) * 2
        for kk in range(2):
            for cp in w_copies(q + kk):
                cp.wait()
            d = jnp.dot(xv[kk], wbuf[kk], preferred_element_type=F32)
            if kk == 0:
                acc[...] = d
            else:
                t = acc[...] + d
                h = jax.nn.silu(t[:, :GN]) * t[:, GN:]
                hv[lax.rem(c, 2), :, pl.ds(pl.multiple_of(n * GN, GN), GN)] = h.astype(BF16)
            w_start(q + kk + 2)

    def s0_copy(u, c, k, j):
        s1, s2, _ = bits(k)
        i1 = jnp.where(j < 2, 1 - s1, s1)
        i2 = jnp.where(lax.rem(j, 2) == 0, 1 - s2, s2)
        i = i1 * 2 + i2
        slot = lax.rem(u, 3)
        return pltpu.make_async_remote_copy(
            st0.at[slot], rv0.at[k, i], s0s.at[slot], r0.at[k, i], **to(core_peer))

    def r0_wait(k, i):
        pltpu.make_async_remote_copy(st0.at[0], rv0.at[k, i], s0s.at[0], r0.at[k, i], **to(core_peer)).wait_recv()

    def s0(c, u0, j0, step0):
        def body(t, _):
            k, j = t // 2, j0 + lax.rem(t, 2)
            u = c * 12 + u0 + t
            slot = d_next(step0 + t)
            y = jnp.dot(hv[lax.rem(c, 2)], dbuf[slot], preferred_element_type=F32)

            @pl.when(u >= 3)
            def _():
                s0_copy(u, c, k, j).wait_send()

            st0[lax.rem(u, 3)] = y.astype(BF16)
            s0_copy(u, c, k, j).start()
            return 0

        lax.fori_loop(0, 6, body, 0)

    def s1_copy(k, j):
        s1, s2, _ = bits(k)
        i2 = jnp.where(j == 0, 1 - s2, s2)
        return pltpu.make_async_remote_copy(
            st1.at[k, j], rv1.at[k, i2], s1s.at[k, j], r1.at[k, i2], **to(peer(dim(k, 0))))

    def r1_wait(k, i2):
        pltpu.make_async_remote_copy(
            st1.at[k, 0], rv1.at[k, i2], s1s.at[k, 0], r1.at[k, i2], **to(peer(dim(k, 0)))).wait_recv()

    def s1(c, step0):
        def body(t, _):
            k, j = t // 2, lax.rem(t, 2)
            b1, b2, _ = bits(k)
            i2 = jnp.where(j == 0, 1 - b2, b2)
            i = (1 - b1) * 2 + i2
            slot = d_next(step0 + t)
            y = jnp.dot(hv[lax.rem(c, 2)], dbuf[slot], preferred_element_type=F32)
            r0_wait(k, i)

            @pl.when(c > 0)
            def _():
                s1_copy(k, j).wait_send()

            st1[k, j] = (y + rv0[k, i].astype(F32)).astype(BF16)
            s1_copy(k, j).start()
            return 0

        lax.fori_loop(0, 6, body, 0)

    def s2_copy(k):
        return pltpu.make_async_remote_copy(
            st2.at[k], rv2.at[k], s2s.at[k], r2.at[k], **to(peer(dim(k, 1))))

    def s2(c):
        def body(k, _):
            b1, b2, _ = bits(k)
            i = b1 * 2 + 1 - b2
            slot = d_next(c * WD_STEPS + 18 + k)
            y = jnp.dot(hv[lax.rem(c, 2)], dbuf[slot], preferred_element_type=F32)
            r0_wait(k, i)
            r1_wait(k, 1 - b2)

            @pl.when(c > 0)
            def _():
                s2_copy(k).wait_send()

            st2[k] = (y + rv0[k, i].astype(F32) + rv1[k, 1 - b2].astype(F32)).astype(BF16)
            s2_copy(k).start()
            return 0

        lax.fori_loop(0, 3, body, 0)

    def s3_copy(k):
        return pltpu.make_async_remote_copy(
            st3.at[k], rv3.at[k], s3s.at[k], r3.at[k], **to(peer(dim(k, 2))))

    def held(k, half):
        b1, b2, _ = bits(k)
        part = pl.ds(pl.multiple_of(half * HALF, HALF), HALF)
        return (rv0[k, b1 * 2 + b2, part].astype(F32) + rv1[k, b2, part].astype(F32)
                + rv2[k, part].astype(F32))

    def s3(c):
        def body(k, _):
            b1, b2, b3 = bits(k)
            slot = d_next(c * WD_STEPS + 21 + k)
            part = pl.ds(pl.multiple_of((1 - b3) * HALF, HALF), HALF)
            y = jnp.dot(hv[lax.rem(c, 2), part], dbuf[slot], preferred_element_type=F32)
            r0_wait(k, b1 * 2 + b2)
            r1_wait(k, b2)
            s2_copy(k).wait_recv()

            @pl.when(c > 0)
            def _():
                s3_copy(k).wait_send()

            st3[k] = (y + held(k, 1 - b3)).astype(BF16)
            s3_copy(k).start()
            return 0

        lax.fori_loop(0, 3, body, 0)

    def place(c, k, i1, i2, half):
        return y_hbm.at[pl.ds(pl.multiple_of(c * R + half * HALF, HALF), HALF), pl.ds(col(k, b0, i1, i2), CB)]

    def f_copies(c, k):
        b1, b2, b3 = bits(k)
        par = lax.rem(c, 2)
        dst = place(c, k, b1, b2, b3)
        return [
            pltpu.make_async_remote_copy(stf.at[k], dst, fs.at[k, 0], g3.at[par, k], **to(peer(dim(k, 2)))),
            pltpu.make_async_remote_copy(stf.at[k], dst, fs.at[k, 1], g2.at[par, k, 0], **to(peer(dim(k, 1)))),
            pltpu.make_async_remote_copy(stf.at[k], dst, fs.at[k, 2], g1.at[par, k, 0], **to(peer(dim(k, 0)))),
            pltpu.make_async_remote_copy(stf.at[k], dst, fs.at[k, 3], g0.at[c, k], **to(core_peer)),
        ]

    def f_local(c, k):
        b1, b2, b3 = bits(k)
        return pltpu.make_async_copy(stf.at[k], place(c, k, b1, b2, b3), fl.at[k])

    def f_wait(c):
        def body(k, _):
            f_local(c, k).wait()
            for cp in f_copies(c, k):
                cp.wait_send()
            return 0

        lax.fori_loop(0, 3, body, 0)

    def fin(c):
        @pl.when(c > 0)
        def _():
            f_wait(c - 1)

        def body(k, _):
            b1, b2, b3 = bits(k)
            slot = d_next(c * WD_STEPS + 24 + k)
            part = pl.ds(pl.multiple_of(b3 * HALF, HALF), HALF)
            y = jnp.dot(hv[lax.rem(c, 2), part], dbuf[slot], preferred_element_type=F32)
            s3_copy(k).wait_recv()
            stf[k] = (y + held(k, b3) + rv3[k].astype(F32)).astype(BF16)
            for cp in f_copies(c, k):
                cp.start()
            f_local(c, k).start()
            return 0

        lax.fori_loop(0, 3, body, 0)

        @pl.when(c < nc - 1)
        def _():
            for i, dev in enumerate(everyone):
                pl.semaphore_signal(credit.at[i], inc=1, **to(dev))

    def a3_copies(c, k):
        b1, b2, b3 = bits(k)
        par = lax.rem(c, 2)
        p = place(c, k, b1, b2, 1 - b3)
        return [
            pltpu.make_async_remote_copy(p, p, a3s.at[k, 0], g2.at[par, k, 1], **to(peer(dim(k, 1)))),
            pltpu.make_async_remote_copy(p, p, a3s.at[k, 1], g1.at[par, k, 1], **to(peer(dim(k, 0)))),
            pltpu.make_async_remote_copy(p, p, a3s.at[k, 2], g0.at[c, k], **to(core_peer)),
        ]

    def a2_copies(c, k, i):
        b1, b2, b3 = bits(k)
        par = lax.rem(c, 2)
        p = place(c, k, b1, 1 - b2, b3 if i == 0 else 1 - b3)
        return [
            pltpu.make_async_remote_copy(p, p, a2s.at[k, i, 0], g1.at[par, k, 2 + i], **to(peer(dim(k, 0)))),
            pltpu.make_async_remote_copy(p, p, a2s.at[k, i, 1], g0.at[c, k], **to(core_peer)),
        ]

    def a1_copies(c, k, i):
        b1, b2, b3 = bits(k)
        p = place(c, k, 1 - b1, b2 if i < 2 else 1 - b2, b3 if i % 2 == 0 else 1 - b3)
        return [pltpu.make_async_remote_copy(p, p, a1s.at[k, i], g0.at[c, k], **to(core_peer))]

    def landed(sem, p):
        pltpu.make_async_remote_copy(p, p, a1s.at[0, 0], sem, **to(core_peer)).wait_recv()

    def a3_wait(c):
        def body(k, _):
            for cp in a3_copies(c, k):
                cp.wait_send()
            return 0

        lax.fori_loop(0, 3, body, 0)

    def a3(c):
        @pl.when(c > 0)
        def _():
            a3_wait(c - 1)

        def body(k, _):
            b1, b2, b3 = bits(k)
            landed(g3.at[lax.rem(c, 2), k], place(c, k, b1, b2, 1 - b3))
            for cp in a3_copies(c, k):
                cp.start()
            return 0

        lax.fori_loop(0, 3, body, 0)

    def a2_wait(c):
        def body(k, _):
            for i in range(2):
                for cp in a2_copies(c, k, i):
                    cp.wait_send()
            return 0

        lax.fori_loop(0, 3, body, 0)

    def a2(c):
        @pl.when(c > 0)
        def _():
            a2_wait(c - 1)

        for i in range(2):
            def body(k, _):
                b1, b2, b3 = bits(k)
                landed(g2.at[lax.rem(c, 2), k, i], place(c, k, b1, 1 - b2, b3 if i == 0 else 1 - b3))
                for cp in a2_copies(c, k, i):
                    cp.start()
                return 0

            lax.fori_loop(0, 3, body, 0)

    def a1_wait(c):
        def body(k, _):
            for i in range(4):
                for cp in a1_copies(c, k, i):
                    cp.wait_send()
            return 0

        lax.fori_loop(0, 3, body, 0)

    def a1(c):
        @pl.when(c > 0)
        def _():
            a1_wait(c - 1)

        for i in range(4):
            def body(k, _):
                b1, b2, b3 = bits(k)
                landed(g1.at[lax.rem(c, 2), k, i],
                       place(c, k, 1 - b1, b2 if i < 2 else 1 - b2, b3 if i % 2 == 0 else 1 - b3))
                for cp in a1_copies(c, k, i):
                    cp.start()
                return 0

            lax.fori_loop(0, 3, body, 0)

    def a0_wait(c):
        def body(k, _):
            p = y_hbm.at[pl.ds(pl.multiple_of(c * R, R), R), pl.ds(col(k, 1 - b0, 0, 0), 4 * CB)]
            landed(g0.at[c, k], p)
            return 0

        lax.fori_loop(0, 3, body, 0)

    def chunk(c, _):
        @pl.when(c < nc)
        def _():
            for cp in x_copies(c):
                cp.wait()

        def tile(n, _):
            @pl.when(c < nc)
            def _():
                gate_up(c, n)

            @pl.when((n == 0) & (c >= 2))
            def _():
                a1(c - 2)

            late = (c >= 1) & (c <= nc)
            for slot, act in SLOTS:
                @pl.when(late & (n == slot))
                def _(act=act):
                    {"s2": s2, "s3": s3, "fin": fin, "a3": a3, "a2": a2}[act](c - 1)

            return 0

        lax.fori_loop(0, nt, tile, 0)

        @pl.when(c < nc)
        def _():
            @pl.when(c < nc - 1)
            def _():
                for cp in x_copies(c + 1):
                    cp.start()

            @pl.when(c > 0)
            def _():
                for i in range(4):
                    pl.semaphore_wait(credit.at[i], 1)

            s0(c, 0, 0, c * WD_STEPS)
            s1(c, c * WD_STEPS + 6)
            s0(c, 6, 2, c * WD_STEPS + 12)

        return 0

    lax.fori_loop(0, nc + 2, chunk, 0)

    last = nc - 1
    for slot in range(3):
        s0_copy(slot, last, 0, 0).wait_send()

    def drain(k, _):
        for j in range(2):
            s1_copy(k, j).wait_send()
        s2_copy(k).wait_send()
        s3_copy(k).wait_send()
        return 0

    lax.fori_loop(0, 3, drain, 0)
    f_wait(last)
    a3_wait(last)
    a2_wait(last)
    a1_wait(last)

    def land(c, _):
        a0_wait(c)
        return 0

    lax.fori_loop(0, nc, land, 0)


SLOTS = ((1, "s2"), (2, "s3"), (3, "fin"), (5, "a3"), (6, "a2"))


def block(x, wg, wu, wd):
    rows, depth = x.shape
    units = wg.shape[1]
    nc = rows // R
    dma, vmem = pltpu.SemaphoreType.DMA, pltpu.VMEM
    return pl.pallas_call(
        kernel,
        name="mlp",
        out_shape=jax.ShapeDtypeStruct((rows, depth), BF16),
        in_specs=[pl.BlockSpec(memory_space=pl.ANY)] * 4,
        out_specs=pl.BlockSpec(memory_space=pl.ANY),
        scratch_shapes=[
            vmem((2, R, KB), BF16),
            vmem((2, KB, 2 * GN), BF16),
            vmem((R, 2 * GN), F32),
            vmem((2, R, units), BF16),
            vmem((3, units, CB), BF16),
            vmem((3, 4, R, CB), BF16),
            vmem((3, 2, R, CB), BF16),
            vmem((3, R, CB), BF16),
            vmem((3, HALF, CB), BF16),
            vmem((3, R, CB), BF16),
            vmem((3, 2, R, CB), BF16),
            vmem((3, R, CB), BF16),
            vmem((3, HALF, CB), BF16),
            vmem((3, HALF, CB), BF16),
            dma((2,)), dma((2, 2)), dma((3,)),
            dma((3,)), dma((3, 2)), dma((3,)), dma((3,)), dma((3, 4)), dma((3,)), dma((3, 3)), dma((3, 2, 2)), dma((3, 4)),
            dma((3, 4)), dma((3, 2)), dma((3,)), dma((3,)),
            dma((2, 3)), dma((2, 3, 2)), dma((2, 3, 4)), dma((nc, 3)),
            pltpu.SemaphoreType.REGULAR((4,)),
        ],
        compiler_params=pltpu.CompilerParams(
            collective_id=0, has_side_effects=True, vmem_limit_bytes=67_043_328
        ),
    )(x, wg, wu, wd)


def solution(mesh):
    return jax.shard_map(
        block,
        mesh=mesh,
        in_specs=(P("dp", None), P(None, "tp"), P(None, "tp"), P("tp", None)),
        out_specs=P("dp", None),
        check_vma=False,
    )
```

```python
import jax
import jax.numpy as jnp
from jax import lax
from jax.experimental import pallas as pl
from jax.experimental.pallas import tpu as pltpu
from jax.sharding import PartitionSpec as P

MESH = pl.DeviceIdType.MESH
F32, BF16 = jnp.float32, jnp.bfloat16

BIG = 352
CB = 512
PACKETS = 2
W_SLOTS = 3
GN = 256
D_STEPS = 12

SLOTS = ((0, "s2", 1), (1, "a3", 2), (3, "s3", 1), (4, "a2", 2), (5, "fin", 1), (6, "a1", 2))


def kernel(x_hbm, wg_hbm, wu_hbm, wd_hbm, y_hbm,
           xv, wbuf, acc, hv, dbuf, rv0, rv1, rv2, rv3, st, st3, stf,
           x_sem, w_sem, d_sem, s0s, s1s, s2s, s3s, fs, fl, a3s, a2s, a1s,
           r0, r1, r2, r3, g3, g2, g1, g0, credit):
    rows, depth = x_hbm.shape
    units = wg_hbm.shape[1]
    kb = depth // PACKETS
    nt = units // GN
    nb = rows // BIG
    nc = nb + 1
    me = lax.axis_index("tp")
    b0 = lax.rem(me, 2)

    def mask(d):
        return jnp.where(d == 0, 8, jnp.where(d == 1, 4, 2))

    def bit(d):
        return lax.rem(me // mask(d), 2)

    def peer(d):
        m = mask(d)
        return me + m - 2 * m * bit(d)

    core_peer = me + 1 - 2 * b0

    def dim(k, s):
        return lax.rem(k + s, 3)

    def bits(k):
        return bit(dim(k, 0)), bit(dim(k, 1)), bit(dim(k, 2))

    def col(k, i0, i1, i2):
        return pl.multiple_of((k * 8 + i0 * 4 + i1 * 2 + i2) * CB, CB)

    def to(dev):
        return dict(device_id={"tp": dev}, device_id_type=MESH)

    def loop(n, body):
        def step(i, _):
            body(i)
            return 0

        lax.fori_loop(0, n, step, 0)

    def w_copies(q):
        n, kk, slot = lax.rem(q // PACKETS, nt), lax.rem(q, PACKETS), lax.rem(q, W_SLOTS)
        src = (pl.ds(pl.multiple_of(kk * kb, kb), kb), pl.ds(pl.multiple_of(n * GN, GN), GN))
        return [
            pltpu.make_async_copy(wg_hbm.at[src], wbuf.at[slot, :, pl.ds(0, GN)], w_sem.at[slot, 0]),
            pltpu.make_async_copy(wu_hbm.at[src], wbuf.at[slot, :, pl.ds(GN, GN)], w_sem.at[slot, 1]),
        ]

    def w_next(q):
        for cp in w_copies(q):
            cp.wait()

        @pl.when(q + W_SLOTS - 1 < nc * nt * PACKETS)
        def _():
            for cp in w_copies(q + W_SLOTS - 1):
                cp.start(priority=1)

        return lax.rem(q, W_SLOTS)

    def d_copy(step):
        r, slot = lax.rem(step, D_STEPS), lax.rem(step, 3)
        k, group = lax.rem(r, 3), r // 3
        b1, _, _ = bits(k)
        i0 = jnp.where((group == 0) | (group == 2), 1 - b0, b0)
        i1 = jnp.where(group < 2, 1 - b1, b1)
        return pltpu.make_async_copy(
            wd_hbm.at[:, pl.ds(pl.multiple_of(col(k, i0, i1, 0), 2 * CB), 2 * CB)], dbuf.at[slot], d_sem.at[slot])

    def d_next(step):
        d_copy(step).wait()
        d_copy(step + 2).start()
        return lax.rem(step, 3)

    class Chunk:
        def __init__(self, R):
            self.R, self.half = R, R // 2

        def x_copy(self, c, i):
            return pltpu.make_async_copy(
                x_hbm.at[pl.ds(pl.multiple_of(c * BIG, 32), self.R), pl.ds(i * kb, kb)],
                xv.at[i, pl.ds(0, self.R)], x_sem.at[i])

        def gu_epilogue(self, c, n):
            t = acc[pl.ds(0, self.R)]
            h = jax.nn.silu(t[:, :GN]) * t[:, GN:]
            hv[lax.rem(c, 2), pl.ds(0, self.R), pl.ds(pl.multiple_of(n * GN, GN), GN)] = h.astype(BF16)

        def gate_up(self, c, n):
            for i in range(PACKETS):
                pl.when(n == 0)(lambda i=i: self.x_copy(c, i).wait())
                slot = w_next((c * nt + n) * PACKETS + i)
                if i == 0:
                    self.gu_epilogue(c, lax.rem(n + nt - 1, nt))
                d = jnp.dot(xv[i, pl.ds(0, self.R)], wbuf[slot], preferred_element_type=F32)
                acc[pl.ds(0, self.R)] = d if i == 0 else acc[pl.ds(0, self.R)] + d
                pl.when(n == nt - 1)(lambda i=i: either(c + 1, lambda a: a.x_copy(c + 1, i).start(priority=1)))

        def down(self, c, slot, i2, row, n):
            return jnp.dot(hv[lax.rem(c, 2), pl.ds(row, n)],
                           dbuf[slot, :, pl.ds(pl.multiple_of(i2 * CB, CB), CB)], preferred_element_type=F32)

        def pairs(self, c, step0, ready, sums, staged, send):
            def pair(k):
                slot = d_next(step0 + k)
                _, b2, _ = bits(k)
                ready(k)
                for j in range(2):
                    y = self.down(c, slot, 1 - b2 if j == 0 else b2, 0, self.R)
                    for a in sums(k, j):
                        y = y + a[pl.ds(0, self.R)].astype(F32)
                    st[staged(k, j), pl.ds(0, self.R)] = y.astype(BF16)
                for j in range(2):
                    send(k, j)

            loop(3, pair)

        def whole(self, ref):
            return ref.at[pl.ds(0, self.R)]

        def s0_copy(self, p, k, first, j):
            b1, b2, _ = bits(k)
            i1 = 1 - b1 if first else b1
            i, slot = i1 * 2 + (1 - b2 if j == 0 else b2), lax.rem(p, 2) * 2 + j
            return pltpu.make_async_remote_copy(
                self.whole(st.at[slot]), self.whole(rv0.at[k, i]), s0s.at[slot], r0.at[k, i], **to(core_peer))

        def r0_wait(self, k, i):
            pltpu.make_async_remote_copy(
                self.whole(st.at[0]), self.whole(rv0.at[k, i]), s0s.at[0], r0.at[k, i], **to(core_peer)).wait_recv()

        def s0(self, c, first):
            p0 = 0 if first else 3

            def ready(k):
                def wait(chunk):
                    for j in range(2):
                        chunk.s0_copy(p0 + k, k, first, j).wait_send()

                if first:
                    pl.when(k == 2)(lambda: wait(self))
                    pl.when((k < 2) & (c > 0))(lambda: wait(big))
                else:
                    wait(self)

            self.pairs(c, c * D_STEPS + 2 * p0, ready, lambda k, j: [], lambda k, j: lax.rem(p0 + k, 2) * 2 + j,
                       lambda k, j: self.s0_copy(p0 + k, k, first, j).start())

        def s1_copy(self, k, j):
            _, b2, _ = bits(k)
            i2 = 1 - b2 if j == 0 else b2
            return pltpu.make_async_remote_copy(
                self.whole(st.at[4 + k * 2 + j]), self.whole(rv1.at[k, i2]), s1s.at[k, j], r1.at[k, i2],
                **to(peer(dim(k, 0))))

        def r1_wait(self, k, i2):
            pltpu.make_async_remote_copy(
                self.whole(st.at[4]), self.whole(rv1.at[k, i2]), s1s.at[k, 0], r1.at[k, i2],
                **to(peer(dim(k, 0)))).wait_recv()

        def s1(self, c):
            def index(k, j):
                b1, b2, _ = bits(k)
                return (1 - b1) * 2 + (1 - b2 if j == 0 else b2)

            def ready(k):
                for j in range(2):
                    self.r0_wait(k, index(k, j))
                    pl.when(c > 0)(lambda j=j: big.s1_copy(k, j).wait_send())

            self.pairs(c, c * D_STEPS + 3, ready, lambda k, j: [rv0.at[k, index(k, j)]],
                       lambda k, j: 4 + k * 2 + j, lambda k, j: self.s1_copy(k, j).start())

        def s2_copy(self, k):
            return pltpu.make_async_remote_copy(
                self.whole(st.at[10 + k]), self.whole(rv2.at[k]), s2s.at[k], r2.at[k], **to(peer(dim(k, 1))))

        def s2(self, c):
            def body(k):
                b1, b2, _ = bits(k)
                i = b1 * 2 + 1 - b2
                step = c * D_STEPS + 9 + k
                d_copy(step).wait()
                pl.when(k == 0)(lambda: d_copy(step + 2).start())
                self.r0_wait(k, i)
                self.r1_wait(k, 1 - b2)
                pl.when(c > 0)(lambda: big.s2_copy(k).wait_send())
                y = self.down(c, k, 1 - b2, 0, self.R)
                for a in (rv0.at[k, i], rv1.at[k, 1 - b2]):
                    y = y + a[pl.ds(0, self.R)].astype(F32)
                st[10 + k, pl.ds(0, self.R)] = y.astype(BF16)
                self.s2_copy(k).start()

            loop(3, body)

        def last(self, c, k, part, more, dst):
            b1, b2, _ = bits(k)
            row = pl.multiple_of(part * self.half, 16)
            y = self.down(c, k, b2, row, self.half)
            for a in (rv0.at[k, b1 * 2 + b2], rv1.at[k, b2], rv2.at[k]):
                y = y + a[pl.ds(row, self.half)].astype(F32)
            if more:
                y = y + rv3[k, pl.ds(0, self.half)].astype(F32)
            dst[k, pl.ds(0, self.half)] = y.astype(BF16)

        def s3_copy(self, k):
            n = pl.ds(0, self.half)
            return pltpu.make_async_remote_copy(
                st3.at[k, n], rv3.at[k, n], s3s.at[k], r3.at[k], **to(peer(dim(k, 2))))

        def s3(self, c):
            def body(k):
                b1, b2, b3 = bits(k)
                self.r0_wait(k, b1 * 2 + b2)
                self.r1_wait(k, b2)
                self.s2_copy(k).wait_recv()
                pl.when(c > 0)(lambda: big.s3_copy(k).wait_send())
                self.last(c, k, 1 - b3, False, st3)
                self.s3_copy(k).start()

            loop(3, body)

        def place(self, c, k, i1, i2, part):
            row = pl.multiple_of(c * BIG + part * self.half, 16)
            return y_hbm.at[pl.ds(row, self.half), pl.ds(col(k, b0, i1, i2), CB)]

        def f_copies(self, c, k):
            b1, b2, b3 = bits(k)
            par = lax.rem(c, 2)
            src, dst = stf.at[k, pl.ds(0, self.half)], self.place(c, k, b1, b2, b3)
            return [
                pltpu.make_async_remote_copy(src, dst, fs.at[k, 0], g3.at[par, k], **to(peer(dim(k, 2)))),
                pltpu.make_async_remote_copy(src, dst, fs.at[k, 1], g2.at[par, k, 0], **to(peer(dim(k, 1)))),
                pltpu.make_async_remote_copy(src, dst, fs.at[k, 2], g1.at[par, k, 0], **to(peer(dim(k, 0)))),
                pltpu.make_async_remote_copy(src, dst, fs.at[k, 3], g0.at[c, k], **to(core_peer)),
                pltpu.make_async_copy(src, dst, fl.at[k]),
            ]

        def f_wait(self, c):
            def body(k):
                copies = self.f_copies(c, k)
                for cp in copies[:4]:
                    cp.wait_send()
                copies[4].wait()

            loop(3, body)

        def fin(self, c):
            pl.when(c > 0)(lambda: big.f_wait(c - 1))

            def body(k):
                _, _, b3 = bits(k)
                self.s3_copy(k).wait_recv()
                self.last(c, k, b3, True, stf)
                copies = self.f_copies(c, k)
                copies[0].start()
                copies[4].start()
                pl.when((k < 2) & (c < nc - 1))(lambda: d_copy((c + 1) * D_STEPS + k).start())

            loop(3, body)
            for i in (1, 2, 3):
                loop(3, lambda k, i=i: self.f_copies(c, k)[i].start())

            @pl.when(c < nc - 1)
            def _():
                for i, dev in enumerate(everyone):
                    pl.semaphore_signal(credit.at[i], inc=1, **to(dev))

        def a3_copies(self, c, k):
            b1, b2, b3 = bits(k)
            par = lax.rem(c, 2)
            p = self.place(c, k, b1, b2, 1 - b3)
            return [
                pltpu.make_async_remote_copy(p, p, a3s.at[k, 0], g2.at[par, k, 1], **to(peer(dim(k, 1)))),
                pltpu.make_async_remote_copy(p, p, a3s.at[k, 1], g1.at[par, k, 1], **to(peer(dim(k, 0)))),
                pltpu.make_async_remote_copy(p, p, a3s.at[k, 2], g0.at[c, k], **to(core_peer)),
            ]

        def a2_copies(self, c, k, i):
            b1, b2, b3 = bits(k)
            par = lax.rem(c, 2)
            p = self.place(c, k, b1, 1 - b2, b3 if i == 0 else 1 - b3)
            return [
                pltpu.make_async_remote_copy(p, p, a2s.at[k, i, 0], g1.at[par, k, 2 + i], **to(peer(dim(k, 0)))),
                pltpu.make_async_remote_copy(p, p, a2s.at[k, i, 1], g0.at[c, k], **to(core_peer)),
            ]

        def a1_copies(self, c, k, i):
            b1, b2, b3 = bits(k)
            p = self.place(c, k, 1 - b1, b2 if i < 2 else 1 - b2, b3 if i % 2 == 0 else 1 - b3)
            return [pltpu.make_async_remote_copy(p, p, a1s.at[k, i], g0.at[c, k], **to(core_peer))]

        def landed(self, sem, p):
            pltpu.make_async_remote_copy(p, p, a1s.at[0, 0], sem, **to(core_peer)).wait_recv()

        def sent(self, c, copies):
            def body(k):
                for cp in copies(c, k):
                    cp.wait_send()

            loop(3, body)

        def a3_wait(self, c):
            self.sent(c, self.a3_copies)

        def a2_wait(self, c):
            self.sent(c, lambda c, k: self.a2_copies(c, k, 0) + self.a2_copies(c, k, 1))

        def a1_wait(self, c):
            self.sent(c, lambda c, k: sum((self.a1_copies(c, k, i) for i in range(4)), []))

        def a3(self, c):
            pl.when(c > 0)(lambda: big.a3_wait(c - 1))

            def body(k):
                b1, b2, b3 = bits(k)
                self.landed(g3.at[lax.rem(c, 2), k], self.place(c, k, b1, b2, 1 - b3))
                for cp in self.a3_copies(c, k):
                    cp.start()

            loop(3, body)

        def a2(self, c):
            pl.when(c > 0)(lambda: big.a2_wait(c - 1))
            for i in range(2):
                def body(k, i=i):
                    b1, b2, b3 = bits(k)
                    self.landed(g2.at[lax.rem(c, 2), k, i], self.place(c, k, b1, 1 - b2, b3 if i == 0 else 1 - b3))
                    for cp in self.a2_copies(c, k, i):
                        cp.start()

                loop(3, body)

        def a1(self, c):
            pl.when(c > 0)(lambda: big.a1_wait(c - 1))
            for i in range(4):
                def body(k, i=i):
                    b1, b2, b3 = bits(k)
                    self.landed(g1.at[lax.rem(c, 2), k, i],
                                self.place(c, k, 1 - b1, b2 if i < 2 else 1 - b2, b3 if i % 2 == 0 else 1 - b3))
                    for cp in self.a1_copies(c, k, i):
                        cp.start()

                loop(3, body)

        def a0_wait(self, c):
            def body(k):
                p = y_hbm.at[pl.ds(pl.multiple_of(c * BIG, 32), self.R), pl.ds(col(k, 1 - b0, 0, 0), 4 * CB)]
                self.landed(g0.at[c, k], p)

            loop(3, body)

        def early(self, c):
            self.gu_epilogue(c, nt - 1)

            @pl.when(c > 0)
            def _():
                for i in range(4):
                    pl.semaphore_wait(credit.at[i], 1)

            self.s0(c, True)
            self.s1(c)
            self.s0(c, False)

    big, small = Chunk(BIG), Chunk(rows - nb * BIG)

    def either(c, act):
        pl.when((c >= 0) & (c < nb))(lambda: act(big))
        pl.when(c == nb)(lambda: act(small))

    for i in range(PACKETS):
        for cp in w_copies(i):
            cp.start()
        big.x_copy(0, i).start()
    d_copy(0).start()
    d_copy(1).start()

    barrier = pltpu.get_barrier_semaphore()
    everyone = [peer(0), peer(1), peer(2), core_peer]
    for dev in everyone:
        pl.semaphore_signal(barrier, inc=1, **to(dev))
    pl.semaphore_wait(barrier, 4)

    def chunk(c):
        def tile(n):
            either(c, lambda a: a.gate_up(c, n))
            for slot, act, lag in SLOTS:
                pl.when(n == slot)(lambda act=act, lag=lag: either(c - lag, lambda a: getattr(a, act)(c - lag)))

        loop(nt, tile)
        either(c, lambda a: a.early(c))

    loop(nc + 2, chunk)

    last = nc - 1
    for k in (1, 2):
        for j in range(2):
            small.s0_copy(3 + k, k, False, j).wait_send()

    def drain(k):
        for j in range(2):
            small.s1_copy(k, j).wait_send()
        small.s2_copy(k).wait_send()
        small.s3_copy(k).wait_send()

    loop(3, drain)
    small.f_wait(last)
    small.a3_wait(last)
    small.a2_wait(last)
    small.a1_wait(last)
    loop(nc, lambda c: either(c, lambda a: a.a0_wait(c)))


def block(x, wg, wu, wd):
    rows, depth = x.shape
    units = wg.shape[1]
    nc = rows // BIG + 1
    kb = depth // PACKETS
    dma, vmem = pltpu.SemaphoreType.DMA, pltpu.VMEM
    return pl.pallas_call(
        kernel,
        name="mlp",
        out_shape=jax.ShapeDtypeStruct((rows, depth), BF16),
        in_specs=[pl.BlockSpec(memory_space=pl.ANY)] * 4,
        out_specs=pl.BlockSpec(memory_space=pl.ANY),
        scratch_shapes=[
            vmem((PACKETS, BIG, kb), BF16),
            vmem((W_SLOTS, kb, 2 * GN), BF16),
            vmem((BIG, 2 * GN), F32),
            vmem((2, BIG, units), BF16),
            vmem((3, units, 2 * CB), BF16),
            vmem((3, 4, BIG, CB), BF16),
            vmem((3, 2, BIG, CB), BF16),
            vmem((3, BIG, CB), BF16),
            vmem((3, BIG // 2, CB), BF16),
            vmem((13, BIG, CB), BF16),
            vmem((3, BIG // 2, CB), BF16),
            vmem((3, BIG // 2, CB), BF16),
            dma((PACKETS,)), dma((W_SLOTS, 2)), dma((3,)),
            dma((4,)), dma((3, 2)), dma((3,)), dma((3,)), dma((3, 4)), dma((3,)),
            dma((3, 3)), dma((3, 2, 2)), dma((3, 4)),
            dma((3, 4)), dma((3, 2)), dma((3,)), dma((3,)),
            dma((2, 3)), dma((2, 3, 2)), dma((2, 3, 4)), dma((nc, 3)),
            pltpu.SemaphoreType.REGULAR((4,)),
        ],
        compiler_params=pltpu.CompilerParams(
            collective_id=0, has_side_effects=True, vmem_limit_bytes=67_043_328
        ),
    )(x, wg, wu, wd)


def solution(mesh):
    return jax.shard_map(
        block,
        mesh=mesh,
        in_specs=(P("dp", None), P(None, "tp"), P(None, "tp"), P("tp", None)),
        out_specs=P("dp", None),
        check_vma=False,
    )
```

```python
import jax
import jax.numpy as jnp
from jax import lax
from jax.experimental import pallas as pl
from jax.experimental.pallas import tpu as pltpu
from jax.sharding import PartitionSpec as P

MESH = pl.DeviceIdType.MESH
F32, BF16 = jnp.float32, jnp.bfloat16

BIG = 352
CB = 512
PACKETS = 2
W_SLOTS = 3
GN = 256
D_STEPS = 12

SLOTS = ((1, "s2", 1), (4, "s3", 1), (5, "a2", 2), (8, "fin", 1), (12, "a1", 2), (12, "a3", 1))


def kernel(x_hbm, wg_hbm, wu_hbm, wd_hbm, y_hbm,
           xv, wbuf, acc, hv, dbuf, raw, rv0, rv1, rv2, rv3, st, st3, stf,
           x_sem, w_sem, d_sem, s0s, s1s, s2s, s3s, fs, fl, a3s, a2s, a1s,
           r0, r1, r2, r3, g3, g2, g1, g0, credit):
    rows, depth = x_hbm.shape
    units = wg_hbm.shape[1]
    kb = depth // PACKETS
    nt = units // GN
    nb = rows // BIG
    nc = nb + 1
    me = lax.axis_index("tp")
    b0 = lax.rem(me, 2)

    def mask(d):
        return jnp.where(d == 0, 8, jnp.where(d == 1, 4, 2))

    def bit(d):
        return lax.rem(me // mask(d), 2)

    def peer(d):
        m = mask(d)
        return me + m - 2 * m * bit(d)

    core_peer = me + 1 - 2 * b0

    def dim(k, s):
        return lax.rem(k + s, 3)

    def bits(k):
        return bit(dim(k, 0)), bit(dim(k, 1)), bit(dim(k, 2))

    def col(k, i0, i1, i2):
        return pl.multiple_of((k * 8 + i0 * 4 + i1 * 2 + i2) * CB, CB)

    def to(dev):
        return dict(device_id={"tp": dev}, device_id_type=MESH)

    def loop(n, body):
        def step(i, _):
            body(i)
            return 0

        lax.fori_loop(0, n, step, 0)

    def w_copies(q):
        n, kk, slot = lax.rem(q // PACKETS, nt), lax.rem(q, PACKETS), lax.rem(q, W_SLOTS)
        src = (pl.ds(pl.multiple_of(kk * kb, kb), kb), pl.ds(pl.multiple_of(n * GN, GN), GN))
        return [
            pltpu.make_async_copy(wg_hbm.at[src], wbuf.at[slot, :, pl.ds(0, GN)], w_sem.at[slot, 0]),
            pltpu.make_async_copy(wu_hbm.at[src], wbuf.at[slot, :, pl.ds(GN, GN)], w_sem.at[slot, 1]),
        ]

    def w_next(q):
        for cp in w_copies(q):
            cp.wait()

        @pl.when(q + W_SLOTS - 1 < nc * nt * PACKETS)
        def _():
            for cp in w_copies(q + W_SLOTS - 1):
                cp.start(priority=1)

        return lax.rem(q, W_SLOTS)

    def d_copy(step):
        r, slot = lax.rem(step, D_STEPS), lax.rem(step, 3)
        k, group = lax.rem(r, 3), r // 3
        b1, _, _ = bits(k)
        i0 = jnp.where((group == 0) | (group == 2), 1 - b0, b0)
        i1 = jnp.where(group < 2, 1 - b1, b1)
        return pltpu.make_async_copy(
            wd_hbm.at[:, pl.ds(pl.multiple_of(col(k, i0, i1, 0), 2 * CB), 2 * CB)], dbuf.at[slot], d_sem.at[slot])

    def d_start(step):
        pl.when(step < nc * D_STEPS)(lambda: d_copy(step).start())

    class Chunk:
        def __init__(self, R):
            self.R, self.half = R, R // 2

        def x_copy(self, c, i):
            return pltpu.make_async_copy(
                x_hbm.at[pl.ds(pl.multiple_of(c * BIG, 32), self.R), pl.ds(i * kb, kb)],
                xv.at[i, pl.ds(0, self.R)], x_sem.at[i])

        def gu_epilogue(self, c, n):
            t = acc[pl.ds(0, self.R)]
            h = jax.nn.silu(t[:, :GN]) * t[:, GN:]
            hv[lax.rem(c, 2), pl.ds(0, self.R), pl.ds(pl.multiple_of(n * GN, GN), GN)] = h.astype(BF16)

        def gate_up(self, c, n, i):
            pl.when(n == 0)(lambda: self.x_copy(c, i).wait())
            slot = w_next((c * nt + n) * PACKETS + i)
            if i == 0:
                self.gu_epilogue(c, lax.rem(n + nt - 1, nt))
            d = jnp.dot(xv[i, pl.ds(0, self.R)], wbuf[slot], preferred_element_type=F32)
            acc[pl.ds(0, self.R)] = d if i == 0 else acc[pl.ds(0, self.R)] + d
            if i == 0:
                pl.when(n == nt - 1)(lambda: either(c + 1, lambda a: a.x_copy(c + 1, 0).start(priority=1)))

        def down(self, c, slot, i2):
            return jnp.dot(hv[lax.rem(c, 2), pl.ds(0, self.R)],
                           dbuf[slot, :, pl.ds(pl.multiple_of(i2 * CB, CB), CB)], preferred_element_type=F32)

        def pairs(self, c, step0, ready, sums, staged, send):
            def pair(k):
                _, b2, _ = bits(k)
                d_copy(step0 + k).wait()
                ready(k)
                both = jnp.dot(hv[lax.rem(c, 2), pl.ds(0, self.R)], dbuf[k], preferred_element_type=F32)
                for i2 in range(2):
                    j = jnp.where(b2 == i2, 1, 0)
                    y = both[:, i2 * CB : (i2 + 1) * CB]
                    for a in sums(k, i2):
                        y = y + a[pl.ds(0, self.R)].astype(F32)
                    st[staged(k, j), pl.ds(0, self.R)] = y.astype(BF16)
                for j in range(2):
                    send(k, j)
                d_start(step0 + k + 3)

            loop(3, pair)

        def whole(self, ref):
            return ref.at[pl.ds(0, self.R)]

        def s0_copy(self, k, first, j):
            b1, b2, _ = bits(k)
            i1 = 1 - b1 if first else b1
            i, slot = i1 * 2 + (1 - b2 if j == 0 else b2), k * 2 + j
            return pltpu.make_async_remote_copy(
                self.whole(st.at[slot]), self.whole(rv0.at[k, i]), s0s.at[slot], r0.at[k, i], **to(core_peer))

        def r0_wait(self, k, i):
            pltpu.make_async_remote_copy(
                self.whole(st.at[0]), self.whole(rv0.at[k, i]), s0s.at[0], r0.at[k, i], **to(core_peer)).wait_recv()

        def s0(self, c, first):
            def ready(k):
                def wait(chunk):
                    for j in range(2):
                        chunk.s0_copy(k, first, j).wait_send()

                if first:
                    pl.when(c > 0)(lambda: wait(big))
                else:
                    wait(self)

            self.pairs(c, c * D_STEPS + (0 if first else 6), ready, lambda k, i2: [], lambda k, j: k * 2 + j,
                       lambda k, j: self.s0_copy(k, first, j).start())

        def s1_copy(self, k, j):
            _, b2, _ = bits(k)
            i2 = 1 - b2 if j == 0 else b2
            return pltpu.make_async_remote_copy(
                self.whole(st.at[6 + k * 2 + j]), self.whole(rv1.at[k, i2]), s1s.at[k, j], r1.at[k, i2],
                **to(peer(dim(k, 0))))

        def r1_wait(self, k, i2):
            pltpu.make_async_remote_copy(
                self.whole(st.at[6]), self.whole(rv1.at[k, i2]), s1s.at[k, 0], r1.at[k, i2],
                **to(peer(dim(k, 0)))).wait_recv()

        def s1(self, c):
            def index(k, j):
                b1, b2, _ = bits(k)
                return (1 - b1) * 2 + (1 - b2 if j == 0 else b2)

            def ready(k):
                for j in range(2):
                    self.r0_wait(k, index(k, j))
                    pl.when(c > 0)(lambda j=j: big.s1_copy(k, j).wait_send())

            self.pairs(c, c * D_STEPS + 3, ready, lambda k, i2: [rv0.at[k, (1 - bits(k)[0]) * 2 + i2]],
                       lambda k, j: 6 + k * 2 + j, lambda k, j: self.s1_copy(k, j).start())

        def s2_copy(self, k, i):
            b3 = bits(k)[2]
            part = pl.ds(pl.multiple_of((1 - b3 if i == 0 else b3) * self.half, 16), self.half)
            return pltpu.make_async_remote_copy(
                st.at[12 + k, part], rv2.at[k, part], s2s.at[k, i], r2.at[k, i], **to(peer(dim(k, 1))))

        def s2(self, c):
            def body(k):
                b1, b2, _ = bits(k)
                i = b1 * 2 + 1 - b2
                step = c * D_STEPS + 9 + k
                d_copy(step).wait()
                self.r0_wait(k, i)
                self.r1_wait(k, 1 - b2)
                for j in range(2):
                    pl.when(c > 0)(lambda j=j: big.s2_copy(k, j).wait_send())
                y = self.down(c, k, 1 - b2)
                for a in (rv0.at[k, i], rv1.at[k, 1 - b2]):
                    y = y + a[pl.ds(0, self.R)].astype(F32)
                st[12 + k, pl.ds(0, self.R)] = y.astype(BF16)
                raw[k, pl.ds(0, self.R)] = self.down(c, k, b2)
                for i in range(2):
                    self.s2_copy(k, i).start()
                d_start(step + 3)

            loop(3, body)

        def last(self, k, part, more, dst):
            b1, b2, _ = bits(k)
            rows = pl.ds(pl.multiple_of(part * self.half, 16), self.half)
            y = raw[k, rows]
            for a in (rv0.at[k, b1 * 2 + b2], rv1.at[k, b2], rv2.at[k]):
                y = y + a[rows].astype(F32)
            if more:
                y = y + rv3[k, pl.ds(0, self.half)].astype(F32)
            dst[k, pl.ds(0, self.half)] = y.astype(BF16)

        def s3_copy(self, k):
            n = pl.ds(0, self.half)
            return pltpu.make_async_remote_copy(
                st3.at[k, n], rv3.at[k, n], s3s.at[k], r3.at[k], **to(peer(dim(k, 2))))

        def s3(self, c):
            def body(k):
                b1, b2, b3 = bits(k)
                self.r0_wait(k, b1 * 2 + b2)
                self.r1_wait(k, b2)
                self.s2_copy(k, 0).wait_recv()
                pl.when(c > 0)(lambda: big.s3_copy(k).wait_send())
                self.last(k, 1 - b3, False, st3)
                self.s3_copy(k).start()

            loop(3, body)

        def place(self, c, k, i1, i2, part):
            row = pl.multiple_of(c * BIG + part * self.half, 16)
            return y_hbm.at[pl.ds(row, self.half), pl.ds(col(k, b0, i1, i2), CB)]

        def f_copies(self, c, k):
            b1, b2, b3 = bits(k)
            par = lax.rem(c, 2)
            src, dst = stf.at[k, pl.ds(0, self.half)], self.place(c, k, b1, b2, b3)
            return [
                pltpu.make_async_remote_copy(src, dst, fs.at[k, 0], g3.at[par, k], **to(peer(dim(k, 2)))),
                pltpu.make_async_remote_copy(src, dst, fs.at[k, 1], g2.at[par, k, 0], **to(peer(dim(k, 1)))),
                pltpu.make_async_remote_copy(src, dst, fs.at[k, 2], g1.at[par, k, 0], **to(peer(dim(k, 0)))),
                pltpu.make_async_copy(src, dst, fl.at[k]),
            ]

        def f_wait(self, c):
            def body(k):
                copies = self.f_copies(c, k)
                for cp in copies[:3]:
                    cp.wait_send()

            loop(3, body)

        def fin(self, c):
            pl.when(c > 0)(lambda: big.f_wait(c - 1))

            def body(k):
                _, _, b3 = bits(k)
                self.s2_copy(k, 1).wait_recv()
                self.s3_copy(k).wait_recv()
                self.last(k, b3, True, stf)
                copies = self.f_copies(c, k)
                copies[0].start()
                copies[3].start()

            loop(3, body)
            for i in (1, 2):
                loop(3, lambda k, i=i: self.f_copies(c, k)[i].start())

            @pl.when(c < nc - 1)
            def _():
                for i, dev in enumerate(everyone):
                    pl.semaphore_signal(credit.at[i], inc=1, **to(dev))

        def part_of_y(self, c, col0, width):
            return y_hbm.at[pl.ds(pl.multiple_of(c * BIG, 32), self.R), pl.ds(col0, width)]

        def a3_copies(self, c, k):
            b1, b2, b3 = bits(k)
            par = lax.rem(c, 2)
            p = self.place(c, k, b1, b2, 1 - b3)
            return [
                pltpu.make_async_remote_copy(p, p, a3s.at[k, 0], g2.at[par, k, 1], **to(peer(dim(k, 1)))),
                pltpu.make_async_remote_copy(p, p, a3s.at[k, 1], g1.at[par, k, 1], **to(peer(dim(k, 0)))),
            ]

        def a2_copies(self, c, k):
            b1, b2, _ = bits(k)
            p = self.part_of_y(c, col(k, b0, b1, 1 - b2), CB)
            q = self.part_of_y(c, col(k, b0, b1, 0), 2 * CB)
            return [
                pltpu.make_async_remote_copy(p, p, a2s.at[k, 0], g1.at[lax.rem(c, 2), k, 2], **to(peer(dim(k, 0)))),
                pltpu.make_async_remote_copy(q, q, a2s.at[k, 1], g0.at[c, k, 0], **to(core_peer)),
            ]

        def a1_copies(self, c, k):
            b1, _, _ = bits(k)
            q = self.part_of_y(c, col(k, b0, 1 - b1, 0), 2 * CB)
            return [pltpu.make_async_remote_copy(q, q, a1s.at[k], g0.at[c, k, 1], **to(core_peer))]

        def landed(self, sem, p):
            pltpu.make_async_remote_copy(p, p, a1s.at[0], sem, **to(core_peer)).wait_recv()

        def sent(self, c, copies):
            def body(k):
                for cp in copies(c, k):
                    cp.wait_send()

            loop(3, body)

        def a3_wait(self, c):
            self.sent(c, self.a3_copies)

        def a2_wait(self, c):
            self.sent(c, self.a2_copies)

        def a1_wait(self, c):
            self.sent(c, self.a1_copies)

        def a3(self, c):
            pl.when(c > 0)(lambda: big.a3_wait(c - 1))

            def body(k):
                b1, b2, b3 = bits(k)
                self.landed(g3.at[lax.rem(c, 2), k], self.place(c, k, b1, b2, 1 - b3))
                for cp in self.a3_copies(c, k):
                    cp.start()

            loop(3, body)

        def a2(self, c):
            pl.when(c > 0)(lambda: big.a2_wait(c - 1))

            def body(k):
                b1, b2, b3 = bits(k)
                self.landed(g2.at[lax.rem(c, 2), k, 0], self.place(c, k, b1, 1 - b2, b3))
                self.landed(g2.at[lax.rem(c, 2), k, 1], self.place(c, k, b1, 1 - b2, 1 - b3))
                self.f_copies(c, k)[3].wait()
                for cp in self.a2_copies(c, k):
                    cp.start()

            loop(3, body)

        def a1(self, c):
            pl.when(c > 0)(lambda: big.a1_wait(c - 1))

            def body(k):
                b1, b2, b3 = bits(k)
                for i, part in enumerate((b3, 1 - b3)):
                    self.landed(g1.at[lax.rem(c, 2), k, i], self.place(c, k, 1 - b1, b2, part))
                self.landed(g1.at[lax.rem(c, 2), k, 2], self.part_of_y(c, col(k, b0, 1 - b1, 1 - b2), CB))
                for cp in self.a1_copies(c, k):
                    cp.start()

            loop(3, body)

        def a0_wait(self, c):
            def body(k):
                b1, _, _ = bits(k)
                for i, i1 in enumerate((b1, 1 - b1)):
                    self.landed(g0.at[c, k, i], self.part_of_y(c, col(k, 1 - b0, i1, 0), 2 * CB))

            loop(3, body)

        def early(self, c):
            self.gu_epilogue(c, nt - 1)

            @pl.when(c > 0)
            def _():
                for i in range(4):
                    pl.semaphore_wait(credit.at[i], 1)

            self.s0(c, True)
            self.s1(c)
            either(c + 1, lambda a: a.x_copy(c + 1, 1).start(priority=1))
            self.s0(c, False)

    big, small = Chunk(BIG), Chunk(rows - nb * BIG)

    def either(c, act):
        pl.when((c >= 0) & (c < nb))(lambda: act(big))
        pl.when(c == nb)(lambda: act(small))

    for i in range(PACKETS):
        for cp in w_copies(i):
            cp.start()
        big.x_copy(0, i).start()

    barrier = pltpu.get_barrier_semaphore()
    everyone = [peer(0), peer(1), peer(2), core_peer]
    for dev in everyone:
        pl.semaphore_signal(barrier, inc=1, **to(dev))
    pl.semaphore_wait(barrier, 4)

    def chunk(c):
        def tile(n):
            for i in range(PACKETS):
                either(c, lambda a: a.gate_up(c, n, i))
                if i == 0:
                    @pl.when((c == 0) & (n == 1))
                    def _():
                        for j in range(3):
                            d_copy(j).start()

                for slot, act, lag in SLOTS:
                    if slot % PACKETS == i:
                        pl.when(n == slot // PACKETS)(
                            lambda act=act, lag=lag: either(c - lag, lambda a: getattr(a, act)(c - lag)))

        loop(nt, tile)
        either(c, lambda a: a.early(c))

    loop(nc + 2, chunk)

    last = nc - 1
    def drain(k):
        for j in range(2):
            small.s0_copy(k, False, j).wait_send()
        for j in range(2):
            small.s1_copy(k, j).wait_send()
        for j in range(2):
            small.s2_copy(k, j).wait_send()
        small.s3_copy(k).wait_send()

    loop(3, drain)
    small.f_wait(last)
    small.a3_wait(last)
    small.a2_wait(last)
    small.a1_wait(last)
    loop(nc, lambda c: either(c, lambda a: a.a0_wait(c)))


def block(x, wg, wu, wd):
    rows, depth = x.shape
    units = wg.shape[1]
    nc = rows // BIG + 1
    kb = depth // PACKETS
    dma, vmem = pltpu.SemaphoreType.DMA, pltpu.VMEM
    y = pl.pallas_call(
        kernel,
        name="mlp",
        out_shape=jax.ShapeDtypeStruct((rows, depth), BF16),
        in_specs=[pl.BlockSpec(memory_space=pl.ANY)] * 4,
        out_specs=pl.BlockSpec(memory_space=pl.ANY),
        scratch_shapes=[
            vmem((PACKETS, BIG, kb), BF16),
            vmem((W_SLOTS, kb, 2 * GN), BF16),
            vmem((BIG, 2 * GN), F32),
            vmem((2, BIG, units), BF16),
            vmem((3, units, 2 * CB), BF16),
            vmem((3, BIG, CB), F32),
            vmem((3, 4, BIG, CB), BF16),
            vmem((3, 2, BIG, CB), BF16),
            vmem((3, BIG, CB), BF16),
            vmem((3, BIG // 2, CB), BF16),
            vmem((15, BIG, CB), BF16),
            vmem((3, BIG // 2, CB), BF16),
            vmem((3, BIG // 2, CB), BF16),
            dma((PACKETS,)), dma((W_SLOTS, 2)), dma((3,)),
            dma((6,)), dma((3, 2)), dma((3, 2)), dma((3,)), dma((3, 3)), dma((3,)),
            dma((3, 2)), dma((3, 2)), dma((3,)),
            dma((3, 4)), dma((3, 2)), dma((3, 2)), dma((3,)),
            dma((2, 3)), dma((2, 3, 2)), dma((2, 3, 3)), dma((nc, 3, 2)),
            pltpu.SemaphoreType.REGULAR((4,)),
        ],
        compiler_params=pltpu.CompilerParams(
            collective_id=0, has_side_effects=True, vmem_limit_bytes=67_043_328
        ),
    )(x, wg, wu, wd)

    def put(a, b):
        b[...] = a[...]

    return pl.pallas_call(
        put,
        name="put",
        grid=(rows // 256,),
        out_shape=jax.ShapeDtypeStruct((rows, depth), BF16),
        in_specs=[pl.BlockSpec((256, depth), lambda i: (i, 0))],
        out_specs=pl.BlockSpec((256, depth), lambda i: (i, 0)),
        compiler_params=pltpu.CompilerParams(vmem_limit_bytes=40 * 2**20),
    )(y)


def solution(mesh):
    return jax.shard_map(
        block,
        mesh=mesh,
        in_specs=(P("dp", None), P(None, "tp"), P(None, "tp"), P("tp", None)),
        out_specs=P("dp", None),
        check_vma=False,
    )
```

```python
import jax
import jax.numpy as jnp
from jax import lax
from jax.experimental import pallas as pl
from jax.experimental.pallas import tpu as pltpu
from jax.sharding import PartitionSpec as P

MESH = pl.DeviceIdType.MESH
F32, BF16 = jnp.float32, jnp.bfloat16

BIG = 352
CB = 512
PACKETS = 2
W_SLOTS = 3
GN = 256
STRIP = 32
STRIPS, AHEAD = 8, 6
D_STEPS = 12

SLOTS = ((1, "s2", 1), (4, "s3", 1), (5, "a2", 2), (8, "fin", 1), (12, "a1", 2), (12, "a3", 1))


def kept(depth):
    return W_SLOTS * (depth // PACKETS) * 2 * GN // depth, BIG


def kept_parts(depth, y, wbuf, xv):
    in_w, in_x = kept(depth)
    kb = depth // PACKETS
    per = kb // in_w

    def w_part(i):
        part = pl.ds(pl.multiple_of(lax.rem(i, per) * in_w, 16), in_w)
        return y.at[pl.ds(0, in_w), pl.ds(pl.multiple_of(i * CB, CB), CB)], wbuf.at[i // per, part]

    def x_part(i):
        return y.at[pl.ds(in_w, in_x), pl.ds(pl.multiple_of(i * kb, kb), kb)], xv.at[i]

    return [(depth // CB, w_part), (PACKETS, x_part)]


def kernel(x_hbm, wg_hbm, wu_hbm, wd_hbm, y_hbm, wbuf, xv,
           acc, hv, dbuf, raw, rv0, rv1, rv2, rv3, st,
           x_sem, w_sem, d_sem, s0s, s1s, s2s, s3s, fs, fl, a3s, a2s, a1s,
           r0, r1, r2, r3, g3, g2, g1, g0, k_sem, credit):
    rows, depth = x_hbm.shape
    units = wg_hbm.shape[1]
    kb = depth // PACKETS
    nt = units // GN
    nb = rows // BIG
    nc = nb + 1
    me = lax.axis_index("tp")
    b0 = lax.rem(me, 2)

    def mask(d):
        return jnp.where(d == 0, 8, jnp.where(d == 1, 4, 2))

    def bit(d):
        return lax.rem(me // mask(d), 2)

    def peer(d):
        m = mask(d)
        return me + m - 2 * m * bit(d)

    core_peer = me + 1 - 2 * b0

    def dim(k, s):
        return lax.rem(k + s, 3)

    def bits(k):
        return bit(dim(k, 0)), bit(dim(k, 1)), bit(dim(k, 2))

    def col(k, i0, i1, i2):
        return pl.multiple_of((k * 8 + i0 * 4 + i1 * 2 + i2) * CB, CB)

    def to(dev):
        return dict(device_id={"tp": dev}, device_id_type=MESH)

    def loop(n, body):
        def step(i, _):
            body(i)
            return 0

        lax.fori_loop(0, n, step, 0)

    def w_copies(q):
        n, kk, slot = lax.rem(q // PACKETS, nt), lax.rem(q, PACKETS), lax.rem(q, W_SLOTS)
        src = (pl.ds(pl.multiple_of(kk * kb, kb), kb), pl.ds(pl.multiple_of(n * GN, GN), GN))
        return [
            pltpu.make_async_copy(wg_hbm.at[src], wbuf.at[slot, :, pl.ds(0, GN)], w_sem.at[slot, 0]),
            pltpu.make_async_copy(wu_hbm.at[src], wbuf.at[slot, :, pl.ds(GN, GN)], w_sem.at[slot, 1]),
        ]

    def w_next(q):
        for cp in w_copies(q):
            cp.wait()

        @pl.when(q + W_SLOTS - 1 < nc * nt * PACKETS)
        def _():
            for cp in w_copies(q + W_SLOTS - 1):
                cp.start(priority=1)

        return lax.rem(q, W_SLOTS)

    def d_copy(step):
        r, slot = lax.rem(step, D_STEPS), lax.rem(step, 3)
        k, group = lax.rem(r, 3), r // 3
        b1, _, _ = bits(k)
        i0 = jnp.where((group == 0) | (group == 2), 1 - b0, b0)
        i1 = jnp.where(group < 2, 1 - b1, b1)
        return pltpu.make_async_copy(
            wd_hbm.at[:, pl.ds(pl.multiple_of(col(k, i0, i1, 0), 2 * CB), 2 * CB)], dbuf.at[slot], d_sem.at[slot])

    def d_start(step):
        pl.when(step < nc * D_STEPS)(lambda: d_copy(step).start())

    class Chunk:
        def __init__(self, R):
            self.R, self.half = R, R // 2

        def x_copy(self, c, i):
            return pltpu.make_async_copy(
                x_hbm.at[pl.ds(pl.multiple_of(c * BIG, 32), self.R), pl.ds(i * kb, kb)],
                xv.at[i, pl.ds(0, self.R)], x_sem.at[i])

        def gu_epilogue(self, c, n):
            t = acc[pl.ds(0, self.R)]
            h = jax.nn.silu(t[:, :GN]) * t[:, GN:]
            hv[lax.rem(c, 2), pl.ds(0, self.R), pl.ds(pl.multiple_of(n * GN, GN), GN)] = h.astype(BF16)

        def gate_up(self, c, n, i):
            pl.when(n == 0)(lambda: self.x_copy(c, i).wait())
            slot = w_next((c * nt + n) * PACKETS + i)
            if i == 0:
                self.gu_epilogue(c, lax.rem(n + nt - 1, nt))
            d = jnp.dot(xv[i, pl.ds(0, self.R)], wbuf[slot], preferred_element_type=F32)
            acc[pl.ds(0, self.R)] = d if i == 0 else acc[pl.ds(0, self.R)] + d
            if i == 0:
                pl.when(n == nt - 1)(lambda: either(c + 1, lambda a: a.x_copy(c + 1, 0).start(priority=1)))

        def down(self, c, slot, i2):
            return jnp.dot(hv[lax.rem(c, 2), pl.ds(0, self.R)],
                           dbuf[slot, :, pl.ds(pl.multiple_of(i2 * CB, CB), CB)], preferred_element_type=F32)

        def pairs(self, c, step0, ready, sums, staged, send):
            def pair(k):
                _, b2, _ = bits(k)
                d_copy(step0 + k).wait()
                ready(k)
                both = jnp.dot(hv[lax.rem(c, 2), pl.ds(0, self.R)], dbuf[k], preferred_element_type=F32)
                for i2 in range(2):
                    j = jnp.where(b2 == i2, 1, 0)
                    y = both[:, i2 * CB : (i2 + 1) * CB]
                    for a in sums(k, i2):
                        y = y + a[pl.ds(0, self.R)].astype(F32)
                    st[staged(k, j), pl.ds(0, self.R)] = y.astype(BF16)
                for j in range(2):
                    send(k, j)
                d_start(step0 + k + 3)

            loop(3, pair)

        def whole(self, ref):
            return ref.at[pl.ds(0, self.R)]

        def s0_copy(self, k, first, j):
            b1, b2, _ = bits(k)
            i1 = 1 - b1 if first else b1
            i, slot = i1 * 2 + (1 - b2 if j == 0 else b2), k * 2 + j
            return pltpu.make_async_remote_copy(
                self.whole(st.at[slot]), self.whole(rv0.at[k, i]), s0s.at[slot], r0.at[k, i], **to(core_peer))

        def r0_wait(self, k, i):
            pltpu.make_async_remote_copy(
                self.whole(st.at[0]), self.whole(rv0.at[k, i]), s0s.at[0], r0.at[k, i], **to(core_peer)).wait_recv()

        def s0(self, c, first):
            def ready(k):
                if first:
                    @pl.when(c > 0)
                    def _():
                        for j in range(2):
                            big.s2_copy(k, j).wait_send()
                        big.s0_copy(k, first, 1).wait_send()
                else:
                    for j in range(2):
                        self.s0_copy(k, first, j).wait_send()

            self.pairs(c, c * D_STEPS + (0 if first else 6), ready, lambda k, i2: [], lambda k, j: k * 2 + j,
                       lambda k, j: self.s0_copy(k, first, j).start())

        def s1_copy(self, k, j):
            _, b2, _ = bits(k)
            i2 = 1 - b2 if j == 0 else b2
            return pltpu.make_async_remote_copy(
                self.whole(st.at[6 + k * 2 + j]), self.whole(rv1.at[k, i2]), s1s.at[k, j], r1.at[k, i2],
                **to(peer(dim(k, 0))))

        def r1_wait(self, k, i2):
            pltpu.make_async_remote_copy(
                self.whole(st.at[6]), self.whole(rv1.at[k, i2]), s1s.at[k, 0], r1.at[k, i2],
                **to(peer(dim(k, 0)))).wait_recv()

        def s1(self, c):
            def index(k, j):
                b1, b2, _ = bits(k)
                return (1 - b1) * 2 + (1 - b2 if j == 0 else b2)

            def ready(k):
                for j in range(2):
                    self.r0_wait(k, index(k, j))

                @pl.when(c > 0)
                def _():
                    big.f_wait(c - 1, k, True)
                    big.s1_copy(k, 1).wait_send()

            self.pairs(c, c * D_STEPS + 3, ready, lambda k, i2: [rv0.at[k, (1 - bits(k)[0]) * 2 + i2]],
                       lambda k, j: 6 + k * 2 + j, lambda k, j: self.s1_copy(k, j).start())

        def s2_copy(self, k, i):
            b3 = bits(k)[2]
            part = pl.ds(pl.multiple_of((1 - b3 if i == 0 else b3) * self.half, 16), self.half)
            return pltpu.make_async_remote_copy(
                st.at[k * 2, part], rv2.at[k, part], s2s.at[k, i], r2.at[k, i], **to(peer(dim(k, 1))))

        def s2(self, c):
            def body(k):
                b1, b2, _ = bits(k)
                i = b1 * 2 + 1 - b2
                step = c * D_STEPS + 9 + k
                d_copy(step).wait()
                self.r0_wait(k, i)
                self.r1_wait(k, 1 - b2)
                self.s0_copy(k, False, 0).wait_send()
                y = self.down(c, k, 1 - b2)
                for a in (rv0.at[k, i], rv1.at[k, 1 - b2]):
                    y = y + a[pl.ds(0, self.R)].astype(F32)
                st[k * 2, pl.ds(0, self.R)] = y.astype(BF16)
                raw[k, pl.ds(0, self.R)] = self.down(c, k, b2)
                for i in range(2):
                    self.s2_copy(k, i).start()
                d_start(step + 3)

            loop(3, body)

        def last(self, k, part, more):
            b1, b2, _ = bits(k)
            rows = pl.ds(pl.multiple_of(part * self.half, 16), self.half)
            y = raw[k, rows]
            for a in (rv0.at[k, b1 * 2 + b2], rv1.at[k, b2], rv2.at[k]):
                y = y + a[rows].astype(F32)
            if more:
                y = y + rv3[k, pl.ds(0, self.half)].astype(F32)
            st[6 + k * 2, pl.ds(0, self.half)] = y.astype(BF16)

        def s3_copy(self, k):
            n = pl.ds(0, self.half)
            return pltpu.make_async_remote_copy(
                st.at[6 + k * 2, n], rv3.at[k, n], s3s.at[k], r3.at[k], **to(peer(dim(k, 2))))

        def s3(self, c):
            def body(k):
                b1, b2, b3 = bits(k)
                self.r0_wait(k, b1 * 2 + b2)
                self.r1_wait(k, b2)
                self.s2_copy(k, 0).wait_recv()
                self.s1_copy(k, 0).wait_send()
                self.last(k, 1 - b3, False)
                self.s3_copy(k).start()

            loop(3, body)

        def place(self, c, k, i1, i2, part):
            row = pl.multiple_of(c * BIG + part * self.half, 16)
            return y_hbm.at[pl.ds(row, self.half), pl.ds(col(k, b0, i1, i2), CB)]

        def f_copies(self, c, k):
            b1, b2, b3 = bits(k)
            par = lax.rem(c, 2)
            src, dst = st.at[6 + k * 2, pl.ds(0, self.half)], self.place(c, k, b1, b2, b3)
            return [
                pltpu.make_async_remote_copy(src, dst, fs.at[k, 0], g3.at[par, k], **to(peer(dim(k, 2)))),
                pltpu.make_async_remote_copy(src, dst, fs.at[k, 1], g2.at[par, k, 0], **to(peer(dim(k, 1)))),
                pltpu.make_async_remote_copy(src, dst, fs.at[k, 2], g1.at[par, k, 0], **to(peer(dim(k, 0)))),
                pltpu.make_async_copy(src, dst, fl.at[k]),
            ]

        def f_wait(self, c, k, copies):
            for cp in self.f_copies(c, k)[:3]:
                cp.wait_send()
            if copies:
                self.f_copies(c, k)[3].wait()

        def fin(self, c):
            def body(k):
                _, _, b3 = bits(k)
                self.s2_copy(k, 1).wait_recv()
                self.s3_copy(k).wait_recv()
                self.s3_copy(k).wait_send()
                self.last(k, b3, True)
                copies = self.f_copies(c, k)
                copies[0].start()
                copies[3].start()

            loop(3, body)
            for i in (1, 2):
                loop(3, lambda k, i=i: self.f_copies(c, k)[i].start())

            @pl.when(c < nc - 1)
            def _():
                for i, dev in enumerate(everyone):
                    pl.semaphore_signal(credit.at[i], inc=1, **to(dev))

        def part_of_y(self, c, col0, width):
            return y_hbm.at[pl.ds(pl.multiple_of(c * BIG, 32), self.R), pl.ds(col0, width)]

        def a3_copies(self, c, k):
            b1, b2, b3 = bits(k)
            par = lax.rem(c, 2)
            p = self.place(c, k, b1, b2, 1 - b3)
            return [
                pltpu.make_async_remote_copy(p, p, a3s.at[k, 0], g2.at[par, k, 1], **to(peer(dim(k, 1)))),
                pltpu.make_async_remote_copy(p, p, a3s.at[k, 1], g1.at[par, k, 1], **to(peer(dim(k, 0)))),
            ]

        def a2_copies(self, c, k):
            b1, b2, _ = bits(k)
            p = self.part_of_y(c, col(k, b0, b1, 1 - b2), CB)
            q = self.part_of_y(c, col(k, b0, b1, 0), 2 * CB)
            return [
                pltpu.make_async_remote_copy(p, p, a2s.at[k, 0], g1.at[lax.rem(c, 2), k, 2], **to(peer(dim(k, 0)))),
                pltpu.make_async_remote_copy(q, q, a2s.at[k, 1], g0.at[c, k, 0], **to(core_peer)),
            ]

        def a1_copies(self, c, k):
            b1, _, _ = bits(k)
            q = self.part_of_y(c, col(k, b0, 1 - b1, 0), 2 * CB)
            return [pltpu.make_async_remote_copy(q, q, a1s.at[k], g0.at[c, k, 1], **to(core_peer))]

        def landed(self, sem, p):
            pltpu.make_async_remote_copy(p, p, a1s.at[0], sem, **to(core_peer)).wait_recv()

        def sent(self, c, copies):
            def body(k):
                for cp in copies(c, k):
                    cp.wait_send()

            loop(3, body)

        def a3_wait(self, c):
            self.sent(c, self.a3_copies)

        def a2_wait(self, c):
            self.sent(c, self.a2_copies)

        def a1_wait(self, c):
            self.sent(c, self.a1_copies)

        def a3(self, c):
            pl.when(c > 0)(lambda: big.a3_wait(c - 1))

            def body(k):
                b1, b2, b3 = bits(k)
                self.landed(g3.at[lax.rem(c, 2), k], self.place(c, k, b1, b2, 1 - b3))
                for cp in self.a3_copies(c, k):
                    cp.start()

            loop(3, body)

        def a2(self, c):
            pl.when(c > 0)(lambda: big.a2_wait(c - 1))

            def body(k):
                b1, b2, b3 = bits(k)
                self.landed(g2.at[lax.rem(c, 2), k, 0], self.place(c, k, b1, 1 - b2, b3))
                self.landed(g2.at[lax.rem(c, 2), k, 1], self.place(c, k, b1, 1 - b2, 1 - b3))
                if self is small:
                    self.f_copies(c, k)[3].wait()
                for cp in self.a2_copies(c, k):
                    cp.start()

            loop(3, body)

        def a1(self, c):
            pl.when(c > 0)(lambda: big.a1_wait(c - 1))

            def body(k):
                b1, b2, b3 = bits(k)
                for i, part in enumerate((b3, 1 - b3)):
                    self.landed(g1.at[lax.rem(c, 2), k, i], self.place(c, k, 1 - b1, b2, part))
                self.landed(g1.at[lax.rem(c, 2), k, 2], self.part_of_y(c, col(k, b0, 1 - b1, 1 - b2), CB))
                for cp in self.a1_copies(c, k):
                    cp.start()

            loop(3, body)

        def a0_wait(self, c):
            def body(k):
                b1, _, _ = bits(k)
                for i, i1 in enumerate((b1, 1 - b1)):
                    self.landed(g0.at[c, k, i], self.part_of_y(c, col(k, 1 - b0, i1, 0), 2 * CB))

            loop(3, body)

        def early(self, c):
            self.gu_epilogue(c, nt - 1)

            @pl.when(c > 0)
            def _():
                for i in range(4):
                    pl.semaphore_wait(credit.at[i], 1)

            self.s0(c, True)
            self.s1(c)
            either(c + 1, lambda a: a.x_copy(c + 1, 1).start(priority=1))
            self.s0(c, False)

    big, small = Chunk(BIG), Chunk(rows - nb * BIG)

    def either(c, act):
        pl.when((c >= 0) & (c < nb))(lambda: act(big))
        pl.when(c == nb)(lambda: act(small))

    for i in range(PACKETS):
        for cp in w_copies(i):
            cp.start()
        big.x_copy(0, i).start()

    barrier = pltpu.get_barrier_semaphore()
    everyone = [peer(0), peer(1), peer(2), core_peer]
    for dev in everyone:
        pl.semaphore_signal(barrier, inc=1, **to(dev))
    pl.semaphore_wait(barrier, 4)

    rooms = kept_parts(depth, y_hbm, wbuf, xv)

    def keep(act):
        base = 0
        for count, part in rooms:
            loop(count, lambda i, base=base, part=part: act(pltpu.make_async_copy(*part(i), k_sem.at[base + i])))
            base += count

    def chunk(c):
        def tile(n):
            @pl.when((c == nc) & (n == 1))
            def _():
                loop(nc - 2, lambda i: big.a0_wait(i))
                keep(lambda cp: cp.start())

            for i in range(PACKETS):
                either(c, lambda a: a.gate_up(c, n, i))
                if i == 0:
                    @pl.when((c == 0) & (n == 1))
                    def _():
                        for j in range(3):
                            d_copy(j).start()

                for slot, act, lag in SLOTS:
                    if slot % PACKETS == i:
                        pl.when(n == slot // PACKETS)(
                            lambda act=act, lag=lag: either(c - lag, lambda a: getattr(a, act)(c - lag)))

        loop(nt, tile)
        either(c, lambda a: a.early(c))

    loop(nc + 2, chunk)

    last = nc - 1
    def drain(k):
        small.s0_copy(k, False, 1).wait_send()
        small.s1_copy(k, 1).wait_send()
        for j in range(2):
            small.s2_copy(k, j).wait_send()
        small.f_wait(last, k, False)

    loop(3, drain)
    small.a3_wait(last)
    small.a2_wait(last)
    small.a1_wait(last)
    big.a0_wait(nc - 2)
    small.a0_wait(nc - 1)
    keep(lambda cp: cp.wait())


def block(x, wg, wu, wd):
    rows, depth = x.shape
    units = wg.shape[1]
    nc = rows // BIG + 1
    kb = depth // PACKETS
    dma, vmem = pltpu.SemaphoreType.DMA, pltpu.VMEM
    y, wbuf, xv = pl.pallas_call(
        kernel,
        name="mlp",
        out_shape=[
            jax.ShapeDtypeStruct((rows, depth), BF16),
            vmem((W_SLOTS, kb, 2 * GN), BF16),
            vmem((PACKETS, BIG, kb), BF16),
        ],
        in_specs=[pl.BlockSpec(memory_space=pl.ANY)] * 4,
        out_specs=[pl.BlockSpec(memory_space=pl.ANY)] + [pl.BlockSpec(memory_space=pltpu.VMEM)] * 2,
        scratch_shapes=[
            vmem((BIG, 2 * GN), F32),
            vmem((2, BIG, units), BF16),
            vmem((3, units, 2 * CB), BF16),
            vmem((3, BIG, CB), F32),
            vmem((3, 4, BIG, CB), BF16),
            vmem((3, 2, BIG, CB), BF16),
            vmem((3, BIG, CB), BF16),
            vmem((3, BIG // 2, CB), BF16),
            vmem((12, BIG, CB), BF16),
            dma((PACKETS,)), dma((W_SLOTS, 2)), dma((3,)),
            dma((6,)), dma((3, 2)), dma((3, 2)), dma((3,)), dma((3, 3)), dma((3,)),
            dma((3, 2)), dma((3, 2)), dma((3,)),
            dma((3, 4)), dma((3, 2)), dma((3, 2)), dma((3,)),
            dma((2, 3)), dma((2, 3, 2)), dma((2, 3, 3)), dma((nc, 3, 2)),
            dma((depth // CB + PACKETS,)),
            pltpu.SemaphoreType.REGULAR((4,)),
        ],
        compiler_params=pltpu.CompilerParams(
            collective_id=0, has_side_effects=True, vmem_limit_bytes=75 * 2**19
        ),
    )(x, wg, wu, wd)

    return pl.pallas_call(
        put,
        name="put",
        out_shape=jax.ShapeDtypeStruct((rows, depth), BF16),
        in_specs=[pl.BlockSpec(memory_space=pl.ANY)] + [pl.BlockSpec(memory_space=pltpu.VMEM)] * 2,
        out_specs=pl.BlockSpec(memory_space=pl.ANY),
        scratch_shapes=[
            vmem((STRIPS, STRIP, depth), BF16),
            dma((depth // CB + PACKETS,)),
            dma((STRIPS, 2)),
        ],
        compiler_params=pltpu.CompilerParams(vmem_limit_bytes=7 * 2**20),
    )(y, wbuf, xv)


def put(y_hbm, wbuf, xv, o_hbm, buf, k_sem, sem):
    rows, depth = o_hbm.shape
    first = sum(kept(depth))
    count = (rows - first) // STRIP

    def strip(i):
        part, slot = pl.ds(pl.multiple_of(first + i * STRIP, STRIP), STRIP), lax.rem(i, STRIPS)
        return (pltpu.make_async_copy(y_hbm.at[part], buf.at[slot], sem.at[slot, 0]),
                pltpu.make_async_copy(buf.at[slot], o_hbm.at[part], sem.at[slot, 1]))

    def keep(act):
        base = 0
        for n, part in kept_parts(depth, o_hbm, wbuf, xv):
            def one(i, _, base=base, part=part):
                dst, src = part(i)
                act(pltpu.make_async_copy(src, dst, k_sem.at[base + i]))
                return 0

            lax.fori_loop(0, n, one, 0)
            base += n

    for i in range(AHEAD):
        strip(i)[0].start()
    keep(lambda cp: cp.start())

    def step(i, _):
        strip(i)[0].wait()
        strip(i)[1].start()
        j = i + AHEAD

        @pl.when(j < count)
        def _():
            pl.when(j >= STRIPS)(lambda: strip(j - STRIPS)[1].wait())
            strip(j)[0].start()

        return 0

    lax.fori_loop(0, count, step, 0)
    keep(lambda cp: cp.wait())
    for i in range(count - STRIPS, count):
        strip(i)[1].wait()


def solution(mesh):
    return jax.shard_map(
        block,
        mesh=mesh,
        in_specs=(P("dp", None), P(None, "tp"), P(None, "tp"), P("tp", None)),
        out_specs=P("dp", None),
        check_vma=False,
    )
```

```python
import jax
import jax.numpy as jnp
from jax import lax
from jax.experimental import pallas as pl
from jax.experimental.pallas import tpu as pltpu
from jax.sharding import PartitionSpec as P

MESH = pl.DeviceIdType.MESH
F32, BF16 = jnp.float32, jnp.bfloat16

BIG = 352
CB = 512
PACKETS = 2
W_SLOTS = 3
GN = 256
STRIP = 32
STRIPS, AHEAD = 8, 6
D_STEPS = 12

SLOTS = ((1, "s2", 1), (4, "s3", 1), (5, "a2", 2), (8, "fin", 1), (12, "a1", 2), (12, "a3", 1))


def kept(depth):
    return W_SLOTS * (depth // PACKETS) * 2 * GN // depth, BIG


def kept_parts(depth, y, wbuf, xv):
    in_w, in_x = kept(depth)
    kb = depth // PACKETS
    per = kb // in_w

    def w_part(i):
        part = pl.ds(pl.multiple_of(lax.rem(i, per) * in_w, 16), in_w)
        return y.at[pl.ds(0, in_w), pl.ds(pl.multiple_of(i * CB, CB), CB)], wbuf.at[i // per, part]

    def x_part(i):
        return y.at[pl.ds(in_w, in_x), pl.ds(pl.multiple_of(i * kb, kb), kb)], xv.at[i]

    return [(depth // CB, w_part), (PACKETS, x_part)]


def kernel(x_hbm, wg_hbm, wu_hbm, wd_hbm, y_hbm, wbuf, xv,
           acc, hv, dbuf, raw, rv0, rv1, rv2, rv3, st,
           x_sem, w_sem, d_sem, s0s, s1s, s2s, s3s, fs, fl, a3s, a2s, a1s,
           r0, r1, r2, r3, g3, g2, g1, g0, k_sem, credit):
    rows, depth = x_hbm.shape
    units = wg_hbm.shape[1]
    kb = depth // PACKETS
    nt = units // GN
    nb = rows // BIG
    nc = nb + 1
    me = lax.axis_index("tp")
    b0 = lax.rem(me, 2)

    def mask(d):
        if isinstance(d, int):
            return (8, 4, 2)[d]
        return jnp.where(d == 0, 8, jnp.where(d == 1, 4, 2))

    def bit(d):
        return lax.rem(me // mask(d), 2)

    def peer(d):
        m = mask(d)
        return me + m - 2 * m * bit(d)

    core_peer = me + 1 - 2 * b0

    def dim(k, s):
        return (k + s) % 3 if isinstance(k, int) else lax.rem(k + s, 3)

    def bits(k):
        return bit(dim(k, 0)), bit(dim(k, 1)), bit(dim(k, 2))

    def col(k, i0, i1, i2):
        return pl.multiple_of((k * 8 + i0 * 4 + i1 * 2 + i2) * CB, CB)

    def to(dev):
        return dict(device_id={"tp": dev}, device_id_type=MESH)

    def loop(n, body):
        def step(i, _):
            body(i)
            return 0

        lax.fori_loop(0, n, step, 0)

    def w_copies(n, kk, slot):
        src = (pl.ds(kk * kb, kb), pl.ds(pl.multiple_of(n * GN, GN), GN))
        return [
            pltpu.make_async_copy(wg_hbm.at[src], wbuf.at[slot, :, pl.ds(0, GN)], w_sem.at[slot, 0]),
            pltpu.make_async_copy(wu_hbm.at[src], wbuf.at[slot, :, pl.ds(GN, GN)], w_sem.at[slot, 1]),
        ]

    def w_next(c, n, kk):
        slot = lax.rem((c * nt + n) * PACKETS + kk, W_SLOTS)
        for cp in w_copies(n, kk, slot):
            cp.wait()

        @pl.when((c < nc - 1) | (n < nt - 1))
        def _():
            for cp in w_copies(jnp.where(n == nt - 1, 0, n + 1), kk, jnp.where(slot == 0, W_SLOTS - 1, slot - 1)):
                cp.start(priority=1)

        return slot

    def d_copy(step):
        r, slot = lax.rem(step, D_STEPS), lax.rem(step, 3)
        k, group = lax.rem(r, 3), r // 3
        b1, _, _ = bits(k)
        i0 = jnp.where((group == 0) | (group == 2), 1 - b0, b0)
        i1 = jnp.where(group < 2, 1 - b1, b1)
        return pltpu.make_async_copy(
            wd_hbm.at[:, pl.ds(pl.multiple_of(col(k, i0, i1, 0), 2 * CB), 2 * CB)], dbuf.at[slot], d_sem.at[slot])

    def d_start(step):
        pl.when(step < nc * D_STEPS)(lambda: d_copy(step).start())

    class Chunk:
        def __init__(self, R):
            self.R, self.half = R, R // 2

        def x_copy(self, c, i):
            return pltpu.make_async_copy(
                x_hbm.at[pl.ds(pl.multiple_of(c * BIG, 32), self.R), pl.ds(i * kb, kb)],
                xv.at[i, pl.ds(0, self.R)], x_sem.at[i])

        def gu_epilogue(self, c, n):
            t = acc[pl.ds(0, self.R)]
            h = jax.nn.silu(t[:, :GN]) * t[:, GN:]
            hv[lax.rem(c, 2), pl.ds(0, self.R), pl.ds(pl.multiple_of(n * GN, GN), GN)] = h.astype(BF16)

        def gate_up(self, c, n, i):
            pl.when(n == 0)(lambda: self.x_copy(c, i).wait())
            slot = w_next(c, n, i)
            if i == 0:
                self.gu_epilogue(c, lax.rem(n + nt - 1, nt))
            d = jnp.dot(xv[i, pl.ds(0, self.R)], wbuf[slot], preferred_element_type=F32)
            acc[pl.ds(0, self.R)] = d if i == 0 else acc[pl.ds(0, self.R)] + d
            if i == 0:
                pl.when(n == nt - 1)(lambda: either(c + 1, lambda a: a.x_copy(c + 1, 0).start(priority=1)))

        def down(self, c, slot, i2):
            return jnp.dot(hv[lax.rem(c, 2), pl.ds(0, self.R)],
                           dbuf[slot, :, pl.ds(pl.multiple_of(i2 * CB, CB), CB)], preferred_element_type=F32)

        def pairs(self, c, step0, ready, sums, staged, send):
            def pair(k):
                _, b2, _ = bits(k)
                d_copy(step0 + k).wait()
                ready(k)
                both = jnp.dot(hv[lax.rem(c, 2), pl.ds(0, self.R)], dbuf[k], preferred_element_type=F32)
                for i2 in range(2):
                    j = jnp.where(b2 == i2, 1, 0)
                    y = both[:, i2 * CB : (i2 + 1) * CB]
                    for a in sums(k, i2):
                        y = y + a[pl.ds(0, self.R)].astype(F32)
                    st[staged(k, j), pl.ds(0, self.R)] = y.astype(BF16)
                for j in range(2):
                    send(k, j)
                d_start(step0 + k + 3)

            for k in range(3):
                pair(k)

        def whole(self, ref):
            return ref.at[pl.ds(0, self.R)]

        def s0_copy(self, k, first, j):
            b1, b2, _ = bits(k)
            i1 = 1 - b1 if first else b1
            i, slot = i1 * 2 + (1 - b2 if j == 0 else b2), k * 2 + j
            return pltpu.make_async_remote_copy(
                self.whole(st.at[slot]), self.whole(rv0.at[k, i]), s0s.at[slot], r0.at[k, i], **to(core_peer))

        def r0_wait(self, k, i):
            pltpu.make_async_remote_copy(
                self.whole(st.at[0]), self.whole(rv0.at[k, i]), s0s.at[0], r0.at[k, i], **to(core_peer)).wait_recv()

        def s0(self, c, first):
            def ready(k):
                if first:
                    @pl.when(c > 0)
                    def _():
                        for j in range(2):
                            big.s2_copy(k, j).wait_send()
                        big.s0_copy(k, first, 1).wait_send()
                else:
                    for j in range(2):
                        self.s0_copy(k, first, j).wait_send()

            self.pairs(c, c * D_STEPS + (0 if first else 6), ready, lambda k, i2: [], lambda k, j: k * 2 + j,
                       lambda k, j: self.s0_copy(k, first, j).start())

        def s1_copy(self, k, j):
            _, b2, _ = bits(k)
            i2 = 1 - b2 if j == 0 else b2
            return pltpu.make_async_remote_copy(
                self.whole(st.at[6 + k * 2 + j]), self.whole(rv1.at[k, i2]), s1s.at[k, j], r1.at[k, i2],
                **to(peer(dim(k, 0))))

        def r1_wait(self, k, i2):
            pltpu.make_async_remote_copy(
                self.whole(st.at[6]), self.whole(rv1.at[k, i2]), s1s.at[k, 0], r1.at[k, i2],
                **to(peer(dim(k, 0)))).wait_recv()

        def s1(self, c):
            def index(k, j):
                b1, b2, _ = bits(k)
                return (1 - b1) * 2 + (1 - b2 if j == 0 else b2)

            def ready(k):
                for j in range(2):
                    self.r0_wait(k, index(k, j))

                @pl.when(c > 0)
                def _():
                    big.f_wait(c - 1, k, True)
                    big.s1_copy(k, 1).wait_send()

            self.pairs(c, c * D_STEPS + 3, ready, lambda k, i2: [rv0.at[k, (1 - bits(k)[0]) * 2 + i2]],
                       lambda k, j: 6 + k * 2 + j, lambda k, j: self.s1_copy(k, j).start())

        def s2_copy(self, k, i):
            b3 = bits(k)[2]
            part = pl.ds(pl.multiple_of((1 - b3 if i == 0 else b3) * self.half, 16), self.half)
            return pltpu.make_async_remote_copy(
                st.at[k * 2, part], rv2.at[k, part], s2s.at[k, i], r2.at[k, i], **to(peer(dim(k, 1))))

        def s2(self, c):
            def body(k):
                b1, b2, _ = bits(k)
                i = b1 * 2 + 1 - b2
                step = c * D_STEPS + 9 + k
                d_copy(step).wait()
                self.r0_wait(k, i)
                self.r1_wait(k, 1 - b2)
                self.s0_copy(k, False, 0).wait_send()
                y = self.down(c, k, 1 - b2)
                for a in (rv0.at[k, i], rv1.at[k, 1 - b2]):
                    y = y + a[pl.ds(0, self.R)].astype(F32)
                st[k * 2, pl.ds(0, self.R)] = y.astype(BF16)
                raw[k, pl.ds(0, self.R)] = self.down(c, k, b2)
                for i in range(2):
                    self.s2_copy(k, i).start()
                d_start(step + 3)

            for k in range(3):
                body(k)

        def last(self, k, part, more):
            b1, b2, _ = bits(k)
            rows = pl.ds(pl.multiple_of(part * self.half, 16), self.half)
            y = raw[k, rows]
            for a in (rv0.at[k, b1 * 2 + b2], rv1.at[k, b2], rv2.at[k]):
                y = y + a[rows].astype(F32)
            if more:
                y = y + rv3[k, pl.ds(0, self.half)].astype(F32)
            st[6 + k * 2, pl.ds(0, self.half)] = y.astype(BF16)

        def s3_copy(self, k):
            n = pl.ds(0, self.half)
            return pltpu.make_async_remote_copy(
                st.at[6 + k * 2, n], rv3.at[k, n], s3s.at[k], r3.at[k], **to(peer(dim(k, 2))))

        def s3(self, c):
            def body(k):
                b1, b2, b3 = bits(k)
                self.r0_wait(k, b1 * 2 + b2)
                self.r1_wait(k, b2)
                self.s2_copy(k, 0).wait_recv()
                self.s1_copy(k, 0).wait_send()
                self.last(k, 1 - b3, False)
                self.s3_copy(k).start()

            loop(3, body)

        def place(self, c, k, i1, i2, part):
            row = pl.multiple_of(c * BIG + part * self.half, 16)
            return y_hbm.at[pl.ds(row, self.half), pl.ds(col(k, b0, i1, i2), CB)]

        def f_copies(self, c, k):
            b1, b2, b3 = bits(k)
            par = lax.rem(c, 2)
            src, dst = st.at[6 + k * 2, pl.ds(0, self.half)], self.place(c, k, b1, b2, b3)
            return [
                pltpu.make_async_remote_copy(src, dst, fs.at[k, 0], g3.at[par, k], **to(peer(dim(k, 2)))),
                pltpu.make_async_remote_copy(src, dst, fs.at[k, 1], g2.at[par, k, 0], **to(peer(dim(k, 1)))),
                pltpu.make_async_remote_copy(src, dst, fs.at[k, 2], g1.at[par, k, 0], **to(peer(dim(k, 0)))),
                pltpu.make_async_copy(src, dst, fl.at[k]),
            ]

        def f_wait(self, c, k, copies):
            for cp in self.f_copies(c, k)[:3]:
                cp.wait_send()
            if copies:
                self.f_copies(c, k)[3].wait()

        def fin(self, c):
            def body(k):
                _, _, b3 = bits(k)
                self.s2_copy(k, 1).wait_recv()
                self.s3_copy(k).wait_recv()
                self.s3_copy(k).wait_send()
                self.last(k, b3, True)
                copies = self.f_copies(c, k)
                copies[0].start()
                copies[3].start()

            loop(3, body)
            for i in (1, 2):
                loop(3, lambda k, i=i: self.f_copies(c, k)[i].start())

            @pl.when(c < nc - 1)
            def _():
                for i, dev in enumerate(everyone):
                    pl.semaphore_signal(credit.at[i], inc=1, **to(dev))

        def part_of_y(self, c, col0, width):
            return y_hbm.at[pl.ds(pl.multiple_of(c * BIG, 32), self.R), pl.ds(col0, width)]

        def a3_copies(self, c, k):
            b1, b2, b3 = bits(k)
            par = lax.rem(c, 2)
            p = self.place(c, k, b1, b2, 1 - b3)
            return [
                pltpu.make_async_remote_copy(p, p, a3s.at[k, 0], g2.at[par, k, 1], **to(peer(dim(k, 1)))),
                pltpu.make_async_remote_copy(p, p, a3s.at[k, 1], g1.at[par, k, 1], **to(peer(dim(k, 0)))),
            ]

        def a2_copies(self, c, k):
            b1, b2, b3 = bits(k)
            par = lax.rem(c, 2)
            block = self.part_of_y(c, col(k, b0, b1, 1 - b2), CB)
            pieces = [self.place(c, k, b1, 1 - b2, b3), self.place(c, k, b1, 1 - b2, 1 - b3)]
            q = self.part_of_y(c, col(k, b0, b1, 0), 2 * CB)
            return [
                pltpu.make_async_remote_copy(p, p, a2s.at[k, i], g1.at[par, k, 2 + i], **to(peer(dim(k, 0))))
                for i, p in enumerate(pieces if self is small else [block])
            ] + [pltpu.make_async_remote_copy(q, q, a2s.at[k, 2], g0.at[c, k, 0], **to(core_peer))]

        def a1_parts(self, c, k):
            b1, b2, _ = bits(k)
            if self is small:
                return [self.part_of_y(c, col(k, b0, 1 - b1, i2), CB) for i2 in (b2, 1 - b2)]
            return [self.part_of_y(c, col(k, b0, 1 - b1, 0), 2 * CB)]

        def a1_copies(self, c, k):
            return [pltpu.make_async_remote_copy(q, q, a1s.at[k, i], g0.at[c, k, 1 + i], **to(core_peer))
                    for i, q in enumerate(self.a1_parts(c, k))]

        def landed(self, sem, p):
            pltpu.make_async_remote_copy(p, p, a1s.at[0, 0], sem, **to(core_peer)).wait_recv()

        def sent(self, c, copies):
            def body(k):
                for cp in copies(c, k):
                    cp.wait_send()

            loop(3, body)

        def a3_wait(self, c):
            self.sent(c, self.a3_copies)

        def a2_wait(self, c):
            self.sent(c, self.a2_copies)

        def a1_wait(self, c):
            self.sent(c, self.a1_copies)

        def a3(self, c):
            pl.when(c > 0)(lambda: big.a3_wait(c - 1))

            def body(k):
                b1, b2, b3 = bits(k)
                self.landed(g3.at[lax.rem(c, 2), k], self.place(c, k, b1, b2, 1 - b3))
                for cp in self.a3_copies(c, k):
                    cp.start()

            loop(3, body)

        def a2(self, c):
            pl.when(c > 0)(lambda: big.a2_wait(c - 1))

            def piece(k, i):
                b1, b2, b3 = bits(k)
                self.landed(g2.at[lax.rem(c, 2), k, i], self.place(c, k, b1, 1 - b2, b3 if i == 0 else 1 - b3))

            def first(k):
                self.f_copies(c, k)[3].wait()
                piece(k, 0)
                self.a2_copies(c, k)[0].start()

            def body(k):
                if self is not small:
                    piece(k, 0)
                piece(k, 1)
                for cp in self.a2_copies(c, k)[1 if self is small else 0 :]:
                    cp.start()

            if self is small:
                loop(3, first)
            loop(3, body)

        def a1(self, c):
            pl.when(c > 0)(lambda: big.a1_wait(c - 1))

            def near(k):
                b1, b2, b3 = bits(k)
                for i, part in enumerate((b3, 1 - b3)):
                    self.landed(g1.at[lax.rem(c, 2), k, i], self.place(c, k, 1 - b1, b2, part))

            def far(k):
                b1, b2, b3 = bits(k)
                if self is small:
                    for i, part in enumerate((b3, 1 - b3)):
                        self.landed(g1.at[lax.rem(c, 2), k, 2 + i], self.place(c, k, 1 - b1, 1 - b2, part))
                else:
                    self.landed(g1.at[lax.rem(c, 2), k, 2], self.part_of_y(c, col(k, b0, 1 - b1, 1 - b2), CB))

            def first(k):
                near(k)
                self.a1_copies(c, k)[0].start()

            def body(k):
                if self is not small:
                    near(k)
                far(k)
                self.a1_copies(c, k)[-1].start()

            if self is small:
                loop(3, first)
            loop(3, body)

        def a0_wait(self, c):
            def body(k):
                b1, _, _ = bits(k)
                self.landed(g0.at[c, k, 0], self.part_of_y(c, col(k, 1 - b0, b1, 0), 2 * CB))
                if self is small:
                    _, b2, _ = bits(k)
                    for i, i2 in enumerate((b2, 1 - b2)):
                        self.landed(g0.at[c, k, 1 + i], self.part_of_y(c, col(k, 1 - b0, 1 - b1, i2), CB))
                else:
                    self.landed(g0.at[c, k, 1], self.part_of_y(c, col(k, 1 - b0, 1 - b1, 0), 2 * CB))

            loop(3, body)

        def early(self, c):
            self.gu_epilogue(c, nt - 1)

            @pl.when(c > 0)
            def _():
                for i in range(4):
                    pl.semaphore_wait(credit.at[i], 1)

            self.s0(c, True)
            self.s1(c)
            either(c + 1, lambda a: a.x_copy(c + 1, 1).start(priority=1))
            self.s0(c, False)

    big, small = Chunk(BIG), Chunk(rows - nb * BIG)

    def either(c, act):
        pl.when((c >= 0) & (c < nb))(lambda: act(big))
        pl.when(c == nb)(lambda: act(small))

    for i in range(PACKETS):
        for cp in w_copies(0, i, i):
            cp.start()
        big.x_copy(0, i).start()

    barrier = pltpu.get_barrier_semaphore()
    everyone = [peer(0), peer(1), peer(2), core_peer]
    for dev in everyone:
        pl.semaphore_signal(barrier, inc=1, **to(dev))
    pl.semaphore_wait(barrier, 4)

    rooms = kept_parts(depth, y_hbm, wbuf, xv)

    def keep(act):
        base = 0
        for count, part in rooms:
            loop(count, lambda i, base=base, part=part: act(pltpu.make_async_copy(*part(i), k_sem.at[base + i])))
            base += count

    def chunk(c):
        def tile(n):
            @pl.when((c == nc) & (n == 1))
            def _():
                loop(nc - 2, lambda i: big.a0_wait(i))
                keep(lambda cp: cp.start())

            for i in range(PACKETS):
                either(c, lambda a: a.gate_up(c, n, i))
                if i == 0:
                    pl.when((c == 0) & (n >= 3) & (n < 6))(lambda: d_copy(n - 3).start())

                for slot, act, lag in SLOTS:
                    if slot % PACKETS == i:
                        pl.when(n == slot // PACKETS)(
                            lambda act=act, lag=lag: either(c - lag, lambda a: getattr(a, act)(c - lag)))

        loop(nt, tile)
        either(c, lambda a: a.early(c))

    loop(nc + 2, chunk)

    last = nc - 1
    def drain(k):
        small.s0_copy(k, False, 1).wait_send()
        small.s1_copy(k, 1).wait_send()
        for j in range(2):
            small.s2_copy(k, j).wait_send()
        small.f_wait(last, k, False)

    loop(3, drain)
    small.a3_wait(last)
    small.a2_wait(last)
    small.a1_wait(last)
    big.a0_wait(nc - 2)
    small.a0_wait(nc - 1)
    keep(lambda cp: cp.wait())


def block(x, wg, wu, wd):
    rows, depth = x.shape
    units = wg.shape[1]
    nc = rows // BIG + 1
    kb = depth // PACKETS
    dma, vmem = pltpu.SemaphoreType.DMA, pltpu.VMEM
    y, wbuf, xv = pl.pallas_call(
        kernel,
        name="mlp",
        out_shape=[
            jax.ShapeDtypeStruct((rows, depth), BF16),
            vmem((W_SLOTS, kb, 2 * GN), BF16),
            vmem((PACKETS, BIG, kb), BF16),
        ],
        in_specs=[pl.BlockSpec(memory_space=pl.ANY)] * 4,
        out_specs=[pl.BlockSpec(memory_space=pl.ANY)] + [pl.BlockSpec(memory_space=pltpu.VMEM)] * 2,
        scratch_shapes=[
            vmem((BIG, 2 * GN), F32),
            vmem((2, BIG, units), BF16),
            vmem((3, units, 2 * CB), BF16),
            vmem((3, BIG, CB), F32),
            vmem((3, 4, BIG, CB), BF16),
            vmem((3, 2, BIG, CB), BF16),
            vmem((3, BIG, CB), BF16),
            vmem((3, BIG // 2, CB), BF16),
            vmem((12, BIG, CB), BF16),
            dma((PACKETS,)), dma((W_SLOTS, 2)), dma((3,)),
            dma((6,)), dma((3, 2)), dma((3, 2)), dma((3,)), dma((3, 3)), dma((3,)),
            dma((3, 2)), dma((3, 3)), dma((3, 2)),
            dma((3, 4)), dma((3, 2)), dma((3, 2)), dma((3,)),
            dma((2, 3)), dma((2, 3, 2)), dma((2, 3, 4)), dma((nc, 3, 3)),
            dma((depth // CB + PACKETS,)),
            pltpu.SemaphoreType.REGULAR((4,)),
        ],
        compiler_params=pltpu.CompilerParams(
            collective_id=0, has_side_effects=True, vmem_limit_bytes=75 * 2**19
        ),
    )(x, wg, wu, wd)

    return pl.pallas_call(
        put,
        name="put",
        out_shape=jax.ShapeDtypeStruct((rows, depth), BF16),
        in_specs=[pl.BlockSpec(memory_space=pl.ANY)] + [pl.BlockSpec(memory_space=pltpu.VMEM)] * 2,
        out_specs=pl.BlockSpec(memory_space=pl.ANY),
        scratch_shapes=[
            vmem((STRIPS, STRIP, depth), BF16),
            dma((depth // CB + PACKETS,)),
            dma((STRIPS, 2)),
        ],
        compiler_params=pltpu.CompilerParams(vmem_limit_bytes=7 * 2**20),
    )(y, wbuf, xv)


def put(y_hbm, wbuf, xv, o_hbm, buf, k_sem, sem):
    rows, depth = o_hbm.shape
    first = sum(kept(depth))
    count = (rows - first) // STRIP

    def strip(i):
        part, slot = pl.ds(pl.multiple_of(first + i * STRIP, STRIP), STRIP), lax.rem(i, STRIPS)
        return (pltpu.make_async_copy(y_hbm.at[part], buf.at[slot], sem.at[slot, 0]),
                pltpu.make_async_copy(buf.at[slot], o_hbm.at[part], sem.at[slot, 1]))

    def keep(act):
        base = 0
        for n, part in kept_parts(depth, o_hbm, wbuf, xv):
            def one(i, _, base=base, part=part):
                dst, src = part(i)
                act(pltpu.make_async_copy(src, dst, k_sem.at[base + i]))
                return 0

            lax.fori_loop(0, n, one, 0)
            base += n

    for i in range(AHEAD):
        strip(i)[0].start()
    keep(lambda cp: cp.start())

    def step(i, _):
        strip(i)[0].wait()
        strip(i)[1].start()
        j = i + AHEAD

        @pl.when(j < count)
        def _():
            pl.when(j >= STRIPS)(lambda: strip(j - STRIPS)[1].wait())
            strip(j)[0].start()

        return 0

    lax.fori_loop(0, count, step, 0)
    keep(lambda cp: cp.wait())
    for i in range(count - STRIPS, count):
        strip(i)[1].wait()


def solution(mesh):
    return jax.shard_map(
        block,
        mesh=mesh,
        in_specs=(P("dp", None), P(None, "tp"), P(None, "tp"), P("tp", None)),
        out_specs=P("dp", None),
        check_vma=False,
    )
```

```python
import jax
import jax.numpy as jnp
from jax import lax
from jax.experimental import pallas as pl
from jax.experimental.pallas import tpu as pltpu
from jax.sharding import PartitionSpec as P

MESH = pl.DeviceIdType.MESH
F32, BF16 = jnp.float32, jnp.bfloat16

BIG = 352
CB = 512
PACKETS = 2
W_SLOTS = 3
GN = 256
STRIP = 32
STRIPS, AHEAD = 8, 6
D_STEPS = 12

SLOTS = ((1, "s2", 1), (4, "s3", 1), (5, "a2", 2), (8, "fin", 1), (12, "a1", 2), (12, "a3", 1))


def kept(depth):
    return W_SLOTS * (depth // PACKETS) * 2 * GN // depth, BIG


def kept_parts(depth, y, wbuf, xv):
    in_w, in_x = kept(depth)
    kb = depth // PACKETS
    per = kb // in_w

    def w_part(i):
        part = pl.ds(pl.multiple_of(lax.rem(i, per) * in_w, 16), in_w)
        return y.at[pl.ds(0, in_w), pl.ds(pl.multiple_of(i * CB, CB), CB)], wbuf.at[i // per, part]

    def x_part(i):
        return y.at[pl.ds(in_w, in_x), pl.ds(pl.multiple_of(i * kb, kb), kb)], xv.at[i]

    return [(depth // CB, w_part), (PACKETS, x_part)]


def kernel(x_hbm, wg_hbm, wu_hbm, wd_hbm, y_hbm, wbuf, xv,
           acc, hv, dbuf, raw, rv0, rv1, rv2, rv3, st,
           x_sem, w_sem, d_sem, s0s, s1s, s2s, s3s, fs, fl, a3s, a2s, a1s,
           r0, r1, r2, r3, g3, g2, g1, g0, k_sem, credit):
    rows, depth = x_hbm.shape
    units = wg_hbm.shape[1]
    kb = depth // PACKETS
    nt = units // GN
    nb = rows // BIG
    nc = nb + 1
    me = lax.axis_index("tp")
    b0 = lax.rem(me, 2)

    def mask(d):
        if isinstance(d, int):
            return (8, 4, 2)[d]
        return jnp.where(d == 0, 8, jnp.where(d == 1, 4, 2))

    def bit(d):
        return lax.rem(me // mask(d), 2)

    def peer(d):
        m = mask(d)
        return me + m - 2 * m * bit(d)

    core_peer = me + 1 - 2 * b0

    def dim(k, s):
        return (k + s) % 3 if isinstance(k, int) else lax.rem(k + s, 3)

    def bits(k):
        return bit(dim(k, 0)), bit(dim(k, 1)), bit(dim(k, 2))

    def col(k, i0, i1, i2):
        return pl.multiple_of((k * 8 + i0 * 4 + i1 * 2 + i2) * CB, CB)

    def to(dev):
        return dict(device_id={"tp": dev}, device_id_type=MESH)

    def loop(n, body):
        if n == 3:
            for i in range(n):
                body(i)
            return

        def step(i, _):
            body(i)
            return 0

        lax.fori_loop(0, n, step, 0)

    def w_copies(n, kk, slot):
        src = (pl.ds(kk * kb, kb), pl.ds(pl.multiple_of(n * GN, GN), GN))
        return [
            pltpu.make_async_copy(wg_hbm.at[src], wbuf.at[slot, :, pl.ds(0, GN)], w_sem.at[slot, 0]),
            pltpu.make_async_copy(wu_hbm.at[src], wbuf.at[slot, :, pl.ds(GN, GN)], w_sem.at[slot, 1]),
        ]

    def w_next(c, n, kk):
        slot = lax.rem((c * nt + n) * PACKETS + kk, W_SLOTS)
        for cp in w_copies(n, kk, slot):
            cp.wait()

        @pl.when((c < nc - 1) | (n < nt - 1))
        def _():
            for cp in w_copies(jnp.where(n == nt - 1, 0, n + 1), kk, jnp.where(slot == 0, W_SLOTS - 1, slot - 1)):
                cp.start(priority=1)

        return slot

    def d_copy(step):
        r, slot = lax.rem(step, D_STEPS), lax.rem(step, 3)
        k, group = lax.rem(r, 3), r // 3
        b1, _, _ = bits(k)
        i0 = jnp.where((group == 0) | (group == 2), 1 - b0, b0)
        i1 = jnp.where(group < 2, 1 - b1, b1)
        return pltpu.make_async_copy(
            wd_hbm.at[:, pl.ds(pl.multiple_of(col(k, i0, i1, 0), 2 * CB), 2 * CB)], dbuf.at[slot], d_sem.at[slot])

    def d_start(step):
        pl.when(step < nc * D_STEPS)(lambda: d_copy(step).start())

    class Chunk:
        def __init__(self, R):
            self.R, self.half = R, R // 2

        def x_copy(self, c, i):
            return pltpu.make_async_copy(
                x_hbm.at[pl.ds(pl.multiple_of(c * BIG, 32), self.R), pl.ds(i * kb, kb)],
                xv.at[i, pl.ds(0, self.R)], x_sem.at[i])

        def gu_epilogue(self, c, n):
            t = acc[pl.ds(0, self.R)]
            h = jax.nn.silu(t[:, :GN]) * t[:, GN:]
            hv[lax.rem(c, 2), pl.ds(0, self.R), pl.ds(pl.multiple_of(n * GN, GN), GN)] = h.astype(BF16)

        def gate_up(self, c, n, i):
            pl.when(n == 0)(lambda: self.x_copy(c, i).wait())
            slot = w_next(c, n, i)
            if i == 0:
                self.gu_epilogue(c, lax.rem(n + nt - 1, nt))
            d = jnp.dot(xv[i, pl.ds(0, self.R)], wbuf[slot], preferred_element_type=F32)
            acc[pl.ds(0, self.R)] = d if i == 0 else acc[pl.ds(0, self.R)] + d
            if i == 0:
                pl.when(n == nt - 1)(lambda: either(c + 1, lambda a: a.x_copy(c + 1, 0).start(priority=1)))

        def down(self, c, slot, i2):
            return jnp.dot(hv[lax.rem(c, 2), pl.ds(0, self.R)],
                           dbuf[slot, :, pl.ds(pl.multiple_of(i2 * CB, CB), CB)], preferred_element_type=F32)

        def pairs(self, c, step0, ready, sums, staged, send):
            def pair(k):
                _, b2, _ = bits(k)
                d_copy(step0 + k).wait()
                ready(k)
                both = jnp.dot(hv[lax.rem(c, 2), pl.ds(0, self.R)], dbuf[k], preferred_element_type=F32)
                for i2 in range(2):
                    j = jnp.where(b2 == i2, 1, 0)
                    y = both[:, i2 * CB : (i2 + 1) * CB]
                    for a in sums(k, i2):
                        y = y + a[pl.ds(0, self.R)].astype(F32)
                    st[staged(k, j), pl.ds(0, self.R)] = y.astype(BF16)
                for j in range(2):
                    send(k, j)
                d_start(step0 + k + 3)

            for k in range(3):
                pair(k)

        def whole(self, ref):
            return ref.at[pl.ds(0, self.R)]

        def s0_copy(self, k, first, j):
            b1, b2, _ = bits(k)
            i1 = 1 - b1 if first else b1
            i, slot = i1 * 2 + (1 - b2 if j == 0 else b2), k * 2 + j
            return pltpu.make_async_remote_copy(
                self.whole(st.at[slot]), self.whole(rv0.at[k, i]), s0s.at[slot], r0.at[k, i], **to(core_peer))

        def r0_wait(self, k, i):
            pltpu.make_async_remote_copy(
                self.whole(st.at[0]), self.whole(rv0.at[k, i]), s0s.at[0], r0.at[k, i], **to(core_peer)).wait_recv()

        def s0(self, c, first):
            def ready(k):
                if first:
                    @pl.when(c > 0)
                    def _():
                        for j in range(2):
                            big.s2_copy(k, j).wait_send()
                        big.s0_copy(k, first, 1).wait_send()
                else:
                    for j in range(2):
                        self.s0_copy(k, first, j).wait_send()

            self.pairs(c, c * D_STEPS + (0 if first else 6), ready, lambda k, i2: [], lambda k, j: k * 2 + j,
                       lambda k, j: self.s0_copy(k, first, j).start())

        def s1_copy(self, k, j):
            _, b2, _ = bits(k)
            i2 = 1 - b2 if j == 0 else b2
            return pltpu.make_async_remote_copy(
                self.whole(st.at[6 + k * 2 + j]), self.whole(rv1.at[k, i2]), s1s.at[k, j], r1.at[k, i2],
                **to(peer(dim(k, 0))))

        def r1_wait(self, k, i2):
            pltpu.make_async_remote_copy(
                self.whole(st.at[6]), self.whole(rv1.at[k, i2]), s1s.at[k, 0], r1.at[k, i2],
                **to(peer(dim(k, 0)))).wait_recv()

        def s1(self, c):
            def index(k, j):
                b1, b2, _ = bits(k)
                return (1 - b1) * 2 + (1 - b2 if j == 0 else b2)

            def ready(k):
                for j in range(2):
                    self.r0_wait(k, index(k, j))

                @pl.when(c > 0)
                def _():
                    big.f_wait(c - 1, k, True)
                    big.s1_copy(k, 1).wait_send()

            self.pairs(c, c * D_STEPS + 3, ready, lambda k, i2: [rv0.at[k, (1 - bits(k)[0]) * 2 + i2]],
                       lambda k, j: 6 + k * 2 + j, lambda k, j: self.s1_copy(k, j).start())

        def s2_copy(self, k, i):
            b3 = bits(k)[2]
            part = pl.ds(pl.multiple_of((1 - b3 if i == 0 else b3) * self.half, 16), self.half)
            return pltpu.make_async_remote_copy(
                st.at[k * 2, part], rv2.at[k, part], s2s.at[k, i], r2.at[k, i], **to(peer(dim(k, 1))))

        def s2(self, c):
            def body(k):
                b1, b2, _ = bits(k)
                i = b1 * 2 + 1 - b2
                step = c * D_STEPS + 9 + k
                d_copy(step).wait()
                self.r0_wait(k, i)
                self.r1_wait(k, 1 - b2)
                self.s0_copy(k, False, 0).wait_send()
                y = self.down(c, k, 1 - b2)
                for a in (rv0.at[k, i], rv1.at[k, 1 - b2]):
                    y = y + a[pl.ds(0, self.R)].astype(F32)
                st[k * 2, pl.ds(0, self.R)] = y.astype(BF16)
                raw[k, pl.ds(0, self.R)] = self.down(c, k, b2)
                for i in range(2):
                    self.s2_copy(k, i).start()
                d_start(step + 3)

            for k in range(3):
                body(k)

        def last(self, k, part, more):
            b1, b2, _ = bits(k)
            rows = pl.ds(pl.multiple_of(part * self.half, 16), self.half)
            y = raw[k, rows]
            for a in (rv0.at[k, b1 * 2 + b2], rv1.at[k, b2], rv2.at[k]):
                y = y + a[rows].astype(F32)
            if more:
                y = y + rv3[k, pl.ds(0, self.half)].astype(F32)
            st[6 + k * 2, pl.ds(0, self.half)] = y.astype(BF16)

        def s3_copy(self, k):
            n = pl.ds(0, self.half)
            return pltpu.make_async_remote_copy(
                st.at[6 + k * 2, n], rv3.at[k, n], s3s.at[k], r3.at[k], **to(peer(dim(k, 2))))

        def s3(self, c):
            def body(k):
                b1, b2, b3 = bits(k)
                self.r0_wait(k, b1 * 2 + b2)
                self.r1_wait(k, b2)
                self.s2_copy(k, 0).wait_recv()
                self.s1_copy(k, 0).wait_send()
                self.last(k, 1 - b3, False)
                self.s3_copy(k).start()

            loop(3, body)

        def place(self, c, k, i1, i2, part):
            row = pl.multiple_of(c * BIG + part * self.half, 16)
            return y_hbm.at[pl.ds(row, self.half), pl.ds(col(k, b0, i1, i2), CB)]

        def f_copies(self, c, k):
            b1, b2, b3 = bits(k)
            par = lax.rem(c, 2)
            src, dst = st.at[6 + k * 2, pl.ds(0, self.half)], self.place(c, k, b1, b2, b3)
            return [
                pltpu.make_async_remote_copy(src, dst, fs.at[k, 0], g3.at[par, k], **to(peer(dim(k, 2)))),
                pltpu.make_async_remote_copy(src, dst, fs.at[k, 1], g2.at[par, k, 0], **to(peer(dim(k, 1)))),
                pltpu.make_async_remote_copy(src, dst, fs.at[k, 2], g1.at[par, k, 0], **to(peer(dim(k, 0)))),
                pltpu.make_async_copy(src, dst, fl.at[k]),
            ]

        def f_wait(self, c, k, copies):
            for cp in self.f_copies(c, k)[:3]:
                cp.wait_send()
            if copies:
                self.f_copies(c, k)[3].wait()

        def fin(self, c):
            def body(k):
                _, _, b3 = bits(k)
                self.s2_copy(k, 1).wait_recv()
                self.s3_copy(k).wait_recv()
                self.s3_copy(k).wait_send()
                self.last(k, b3, True)
                copies = self.f_copies(c, k)
                copies[0].start()
                copies[3].start()

            loop(3, body)
            for i in (1, 2):
                loop(3, lambda k, i=i: self.f_copies(c, k)[i].start())

            @pl.when(c < nc - 1)
            def _():
                for i, dev in enumerate(everyone):
                    pl.semaphore_signal(credit.at[i], inc=1, **to(dev))

        def part_of_y(self, c, col0, width):
            return y_hbm.at[pl.ds(pl.multiple_of(c * BIG, 32), self.R), pl.ds(col0, width)]

        def a3_copies(self, c, k):
            b1, b2, b3 = bits(k)
            par = lax.rem(c, 2)
            p = self.place(c, k, b1, b2, 1 - b3)
            return [
                pltpu.make_async_remote_copy(p, p, a3s.at[k, 0], g2.at[par, k, 1], **to(peer(dim(k, 1)))),
                pltpu.make_async_remote_copy(p, p, a3s.at[k, 1], g1.at[par, k, 1], **to(peer(dim(k, 0)))),
            ]

        def a2_copies(self, c, k):
            b1, b2, b3 = bits(k)
            par = lax.rem(c, 2)
            block = self.part_of_y(c, col(k, b0, b1, 1 - b2), CB)
            pieces = [self.place(c, k, b1, 1 - b2, b3), self.place(c, k, b1, 1 - b2, 1 - b3)]
            q = self.part_of_y(c, col(k, b0, b1, 0), 2 * CB)
            return [
                pltpu.make_async_remote_copy(p, p, a2s.at[k, i], g1.at[par, k, 2 + i], **to(peer(dim(k, 0))))
                for i, p in enumerate(pieces if self is small else [block])
            ] + [pltpu.make_async_remote_copy(q, q, a2s.at[k, 2], g0.at[c, k, 0], **to(core_peer))]

        def a1_parts(self, c, k):
            b1, b2, _ = bits(k)
            if self is small:
                return [self.part_of_y(c, col(k, b0, 1 - b1, i2), CB) for i2 in (b2, 1 - b2)]
            return [self.part_of_y(c, col(k, b0, 1 - b1, 0), 2 * CB)]

        def a1_copies(self, c, k):
            return [pltpu.make_async_remote_copy(q, q, a1s.at[k, i], g0.at[c, k, 1 + i], **to(core_peer))
                    for i, q in enumerate(self.a1_parts(c, k))]

        def landed(self, sem, p):
            pltpu.make_async_remote_copy(p, p, a1s.at[0, 0], sem, **to(core_peer)).wait_recv()

        def sent(self, c, copies):
            def body(k):
                for cp in copies(c, k):
                    cp.wait_send()

            loop(3, body)

        def a3_wait(self, c):
            self.sent(c, self.a3_copies)

        def a2_wait(self, c):
            self.sent(c, self.a2_copies)

        def a1_wait(self, c):
            self.sent(c, self.a1_copies)

        def a3(self, c):
            pl.when(c > 0)(lambda: big.a3_wait(c - 1))

            def body(k):
                b1, b2, b3 = bits(k)
                self.landed(g3.at[lax.rem(c, 2), k], self.place(c, k, b1, b2, 1 - b3))
                for cp in self.a3_copies(c, k):
                    cp.start()

            loop(3, body)

        def a2(self, c):
            pl.when(c > 0)(lambda: big.a2_wait(c - 1))

            def piece(k, i):
                b1, b2, b3 = bits(k)
                self.landed(g2.at[lax.rem(c, 2), k, i], self.place(c, k, b1, 1 - b2, b3 if i == 0 else 1 - b3))

            def first(k):
                self.f_copies(c, k)[3].wait()
                piece(k, 0)
                self.a2_copies(c, k)[0].start()

            def body(k):
                if self is not small:
                    piece(k, 0)
                piece(k, 1)
                for cp in self.a2_copies(c, k)[1 if self is small else 0 :]:
                    cp.start()

            if self is small:
                loop(3, first)
            loop(3, body)

        def a1(self, c):
            pl.when(c > 0)(lambda: big.a1_wait(c - 1))

            def near(k):
                b1, b2, b3 = bits(k)
                for i, part in enumerate((b3, 1 - b3)):
                    self.landed(g1.at[lax.rem(c, 2), k, i], self.place(c, k, 1 - b1, b2, part))

            def far(k):
                b1, b2, b3 = bits(k)
                if self is small:
                    for i, part in enumerate((b3, 1 - b3)):
                        self.landed(g1.at[lax.rem(c, 2), k, 2 + i], self.place(c, k, 1 - b1, 1 - b2, part))
                else:
                    self.landed(g1.at[lax.rem(c, 2), k, 2], self.part_of_y(c, col(k, b0, 1 - b1, 1 - b2), CB))

            def first(k):
                near(k)
                self.a1_copies(c, k)[0].start()

            def body(k):
                if self is not small:
                    near(k)
                far(k)
                self.a1_copies(c, k)[-1].start()

            if self is small:
                loop(3, first)
            loop(3, body)

        def a0_wait(self, c):
            def body(k):
                b1, _, _ = bits(k)
                self.landed(g0.at[c, k, 0], self.part_of_y(c, col(k, 1 - b0, b1, 0), 2 * CB))
                if self is small:
                    _, b2, _ = bits(k)
                    for i, i2 in enumerate((b2, 1 - b2)):
                        self.landed(g0.at[c, k, 1 + i], self.part_of_y(c, col(k, 1 - b0, 1 - b1, i2), CB))
                else:
                    self.landed(g0.at[c, k, 1], self.part_of_y(c, col(k, 1 - b0, 1 - b1, 0), 2 * CB))

            loop(3, body)

        def early(self, c):
            self.gu_epilogue(c, nt - 1)

            @pl.when(c > 0)
            def _():
                for i in range(4):
                    pl.semaphore_wait(credit.at[i], 1)

            self.s0(c, True)
            self.s1(c)
            either(c + 1, lambda a: a.x_copy(c + 1, 1).start(priority=1))
            self.s0(c, False)

    big, small = Chunk(BIG), Chunk(rows - nb * BIG)

    def either(c, act):
        pl.when((c >= 0) & (c < nb))(lambda: act(big))
        pl.when(c == nb)(lambda: act(small))

    for i in range(PACKETS):
        for cp in w_copies(0, i, i):
            cp.start()
        big.x_copy(0, i).start()

    barrier = pltpu.get_barrier_semaphore()
    everyone = [peer(0), peer(1), peer(2), core_peer]
    for dev in everyone:
        pl.semaphore_signal(barrier, inc=1, **to(dev))
    pl.semaphore_wait(barrier, 4)

    rooms = kept_parts(depth, y_hbm, wbuf, xv)

    def keep(act):
        base = 0
        for count, part in rooms:
            loop(count, lambda i, base=base, part=part: act(pltpu.make_async_copy(*part(i), k_sem.at[base + i])))
            base += count

    def chunk(c):
        def tile(n):
            @pl.when((c == nc) & (n == 1))
            def _():
                loop(nc - 2, lambda i: big.a0_wait(i))
                keep(lambda cp: cp.start())

            for i in range(PACKETS):
                either(c, lambda a: a.gate_up(c, n, i))
                if i == 0:
                    pl.when((c == 0) & (n >= 3) & (n < 6))(lambda: d_copy(n - 3).start())

                for slot, act, lag in SLOTS:
                    if slot % PACKETS == i:
                        pl.when(n == slot // PACKETS)(
                            lambda act=act, lag=lag: either(c - lag, lambda a: getattr(a, act)(c - lag)))

        loop(nt, tile)
        either(c, lambda a: a.early(c))

    loop(nc + 2, chunk)

    last = nc - 1
    def drain(k):
        small.s0_copy(k, False, 1).wait_send()
        small.s1_copy(k, 1).wait_send()
        for j in range(2):
            small.s2_copy(k, j).wait_send()
        small.f_wait(last, k, False)

    loop(3, drain)
    small.a3_wait(last)
    small.a2_wait(last)
    small.a1_wait(last)
    big.a0_wait(nc - 2)
    small.a0_wait(nc - 1)
    keep(lambda cp: cp.wait())


def block(x, wg, wu, wd):
    rows, depth = x.shape
    units = wg.shape[1]
    nc = rows // BIG + 1
    kb = depth // PACKETS
    dma, vmem = pltpu.SemaphoreType.DMA, pltpu.VMEM
    y, wbuf, xv = pl.pallas_call(
        kernel,
        name="mlp",
        out_shape=[
            jax.ShapeDtypeStruct((rows, depth), BF16),
            vmem((W_SLOTS, kb, 2 * GN), BF16),
            vmem((PACKETS, BIG, kb), BF16),
        ],
        in_specs=[pl.BlockSpec(memory_space=pl.ANY)] * 4,
        out_specs=[pl.BlockSpec(memory_space=pl.ANY)] + [pl.BlockSpec(memory_space=pltpu.VMEM)] * 2,
        scratch_shapes=[
            vmem((BIG, 2 * GN), F32),
            vmem((2, BIG, units), BF16),
            vmem((3, units, 2 * CB), BF16),
            vmem((3, BIG, CB), F32),
            vmem((3, 4, BIG, CB), BF16),
            vmem((3, 2, BIG, CB), BF16),
            vmem((3, BIG, CB), BF16),
            vmem((3, BIG // 2, CB), BF16),
            vmem((12, BIG, CB), BF16),
            dma((PACKETS,)), dma((W_SLOTS, 2)), dma((3,)),
            dma((6,)), dma((3, 2)), dma((3, 2)), dma((3,)), dma((3, 3)), dma((3,)),
            dma((3, 2)), dma((3, 3)), dma((3, 2)),
            dma((3, 4)), dma((3, 2)), dma((3, 2)), dma((3,)),
            dma((2, 3)), dma((2, 3, 2)), dma((2, 3, 4)), dma((nc, 3, 3)),
            dma((depth // CB + PACKETS,)),
            pltpu.SemaphoreType.REGULAR((4,)),
        ],
        compiler_params=pltpu.CompilerParams(
            collective_id=0, has_side_effects=True, vmem_limit_bytes=75 * 2**19
        ),
    )(x, wg, wu, wd)

    return pl.pallas_call(
        put,
        name="put",
        out_shape=jax.ShapeDtypeStruct((rows, depth), BF16),
        in_specs=[pl.BlockSpec(memory_space=pl.ANY)] + [pl.BlockSpec(memory_space=pltpu.VMEM)] * 2,
        out_specs=pl.BlockSpec(memory_space=pl.ANY),
        scratch_shapes=[
            vmem((STRIPS, STRIP, depth), BF16),
            dma((depth // CB + PACKETS,)),
            dma((STRIPS, 2)),
        ],
        compiler_params=pltpu.CompilerParams(vmem_limit_bytes=7 * 2**20),
    )(y, wbuf, xv)


def put(y_hbm, wbuf, xv, o_hbm, buf, k_sem, sem):
    rows, depth = o_hbm.shape
    first = sum(kept(depth))
    count = (rows - first) // STRIP

    def strip(i):
        part, slot = pl.ds(pl.multiple_of(first + i * STRIP, STRIP), STRIP), lax.rem(i, STRIPS)
        return (pltpu.make_async_copy(y_hbm.at[part], buf.at[slot], sem.at[slot, 0]),
                pltpu.make_async_copy(buf.at[slot], o_hbm.at[part], sem.at[slot, 1]))

    def keep(act):
        base = 0
        for n, part in kept_parts(depth, o_hbm, wbuf, xv):
            def one(i, _, base=base, part=part):
                dst, src = part(i)
                act(pltpu.make_async_copy(src, dst, k_sem.at[base + i]))
                return 0

            lax.fori_loop(0, n, one, 0)
            base += n

    for i in range(AHEAD):
        strip(i)[0].start()
    keep(lambda cp: cp.start())

    def step(i, _):
        strip(i)[0].wait()
        strip(i)[1].start()
        j = i + AHEAD

        @pl.when(j < count)
        def _():
            pl.when(j >= STRIPS)(lambda: strip(j - STRIPS)[1].wait())
            strip(j)[0].start()

        return 0

    lax.fori_loop(0, count, step, 0)
    keep(lambda cp: cp.wait())
    for i in range(count - STRIPS, count):
        strip(i)[1].wait()


def solution(mesh):
    return jax.shard_map(
        block,
        mesh=mesh,
        in_specs=(P("dp", None), P(None, "tp"), P(None, "tp"), P("tp", None)),
        out_specs=P("dp", None),
        check_vma=False,
    )
```

```python
import jax
import jax.numpy as jnp
from jax import lax
from jax.experimental import pallas as pl
from jax.experimental.pallas import tpu as pltpu
from jax.sharding import PartitionSpec as P

MESH = pl.DeviceIdType.MESH
F32, BF16 = jnp.float32, jnp.bfloat16

BIG = 352
CB = 512
PACKETS = 2
W_SLOTS = 3
GN = 256
STRIP = 32
STRIPS, AHEAD = 8, 6
D_STEPS = 12

SLOTS = ((1, "s2", 1), (4, "s3", 1), (5, "a2", 2), (8, "fin", 1), (12, "a1", 2), (12, "a3", 1))


def kept(depth):
    return W_SLOTS * (depth // PACKETS) * 2 * GN // depth, BIG


def kept_parts(depth, y, wbuf, xv):
    in_w, in_x = kept(depth)
    kb = depth // PACKETS
    per = kb // in_w

    def w_part(i):
        part = pl.ds(pl.multiple_of(lax.rem(i, per) * in_w, 16), in_w)
        return y.at[pl.ds(0, in_w), pl.ds(pl.multiple_of(i * CB, CB), CB)], wbuf.at[i // per, part]

    def x_part(i):
        return y.at[pl.ds(in_w, in_x), pl.ds(pl.multiple_of(i * kb, kb), kb)], xv.at[i]

    return [(depth // CB, w_part), (PACKETS, x_part)]


def kernel(x_hbm, wg_hbm, wu_hbm, wd_hbm, y_hbm, wbuf, xv,
           acc, hv, dbuf, raw, rv0, rv1, rv2, rv3, st,
           x_sem, w_sem, d_sem, s0s, s1s, s2s, s3s, fs, fl, a3s, a2s, a1s,
           r0, r1, r2, r3, g3, g2, g1, g0, k_sem, credit):
    rows, depth = x_hbm.shape
    units = wg_hbm.shape[1]
    kb = depth // PACKETS
    nt = units // GN
    nb = rows // BIG
    nc = nb + 1
    me = lax.axis_index("tp")
    b0 = lax.rem(me, 2)

    def mask(d):
        if isinstance(d, int):
            return (8, 4, 2)[d]
        return jnp.where(d == 0, 8, jnp.where(d == 1, 4, 2))

    def bit(d):
        return lax.rem(me // mask(d), 2)

    def peer(d):
        m = mask(d)
        return me + m - 2 * m * bit(d)

    core_peer = me + 1 - 2 * b0

    def dim(k, s):
        return (k + s) % 3 if isinstance(k, int) else lax.rem(k + s, 3)

    def bits(k):
        return bit(dim(k, 0)), bit(dim(k, 1)), bit(dim(k, 2))

    def col(k, i0, i1, i2):
        return pl.multiple_of((k * 8 + i0 * 4 + i1 * 2 + i2) * CB, CB)

    def to(dev):
        return dict(device_id={"tp": dev}, device_id_type=MESH)

    def loop(n, body):
        if n == 3:
            for i in range(n):
                body(i)
            return

        def step(i, _):
            body(i)
            return 0

        lax.fori_loop(0, n, step, 0)

    def w_copies(n, kk, slot):
        src = (pl.ds(kk * kb, kb), pl.ds(pl.multiple_of(n * GN, GN), GN))
        return [
            pltpu.make_async_copy(wg_hbm.at[src], wbuf.at[slot, :, pl.ds(0, GN)], w_sem.at[slot, 0]),
            pltpu.make_async_copy(wu_hbm.at[src], wbuf.at[slot, :, pl.ds(GN, GN)], w_sem.at[slot, 1]),
        ]

    def w_next(c, n, kk):
        slot = lax.rem((c * nt + n) * PACKETS + kk, W_SLOTS)
        for cp in w_copies(n, kk, slot):
            cp.wait()

        @pl.when((c < nc - 1) | (n < nt - 1))
        def _():
            for cp in w_copies(jnp.where(n == nt - 1, 0, n + 1), kk, jnp.where(slot == 0, W_SLOTS - 1, slot - 1)):
                cp.start(priority=1)

        return slot

    def d_copy(step):
        r, slot = lax.rem(step, D_STEPS), lax.rem(step, 3)
        k, group = lax.rem(r, 3), r // 3
        b1, _, _ = bits(k)
        i0 = jnp.where((group == 0) | (group == 2), 1 - b0, b0)
        i1 = jnp.where(group < 2, 1 - b1, b1)
        return pltpu.make_async_copy(
            wd_hbm.at[:, pl.ds(pl.multiple_of(col(k, i0, i1, 0), 2 * CB), 2 * CB)], dbuf.at[slot], d_sem.at[slot])

    def d_start(step):
        pl.when(step < nc * D_STEPS)(lambda: d_copy(step).start())

    class Chunk:
        def __init__(self, R):
            self.R, self.half = R, R // 2

        def x_copy(self, c, i):
            return pltpu.make_async_copy(
                x_hbm.at[pl.ds(pl.multiple_of(c * BIG, 32), self.R), pl.ds(i * kb, kb)],
                xv.at[i, pl.ds(0, self.R)], x_sem.at[i])

        def gu_epilogue(self, c, n):
            t = acc[pl.ds(0, self.R)]
            h = jax.nn.silu(t[:, :GN]) * t[:, GN:]
            hv[lax.rem(c, 2), pl.ds(0, self.R), pl.ds(pl.multiple_of(n * GN, GN), GN)] = h.astype(BF16)

        def gate_up(self, c, n, i):
            pl.when(n == 0)(lambda: self.x_copy(c, i).wait())
            slot = w_next(c, n, i)
            if i == 0:
                self.gu_epilogue(c, lax.rem(n + nt - 1, nt))
            d = jnp.dot(xv[i, pl.ds(0, self.R)], wbuf[slot], preferred_element_type=F32)
            acc[pl.ds(0, self.R)] = d if i == 0 else acc[pl.ds(0, self.R)] + d
            if i == 0:
                pl.when(n == nt - 1)(lambda: either(c + 1, lambda a: a.x_copy(c + 1, 0).start(priority=1)))

        def down(self, c, slot, i2):
            return jnp.dot(hv[lax.rem(c, 2), pl.ds(0, self.R)],
                           dbuf[slot, :, pl.ds(pl.multiple_of(i2 * CB, CB), CB)], preferred_element_type=F32)

        def pairs(self, c, step0, ready, sums, staged, send):
            def pair(k):
                _, b2, _ = bits(k)
                d_copy(step0 + k).wait()
                ready(k)
                both = jnp.dot(hv[lax.rem(c, 2), pl.ds(0, self.R)], dbuf[k], preferred_element_type=F32)
                for i2 in range(2):
                    j = jnp.where(b2 == i2, 1, 0)
                    y = both[:, i2 * CB : (i2 + 1) * CB]
                    for a in sums(k, i2):
                        y = y + a[pl.ds(0, self.R)].astype(F32)
                    st[staged(k, j), pl.ds(0, self.R)] = y.astype(BF16)
                for j in range(2):
                    send(k, j)
                d_start(step0 + k + 3)

            for k in range(3):
                pair(k)

        def whole(self, ref):
            return ref.at[pl.ds(0, self.R)]

        def s0_copy(self, k, first, j):
            b1, b2, _ = bits(k)
            i1 = 1 - b1 if first else b1
            i, slot = i1 * 2 + (1 - b2 if j == 0 else b2), k * 2 + j
            return pltpu.make_async_remote_copy(
                self.whole(st.at[slot]), self.whole(rv0.at[k, i]), s0s.at[slot], r0.at[k, i], **to(core_peer))

        def r0_wait(self, k, i):
            pltpu.make_async_remote_copy(
                self.whole(st.at[0]), self.whole(rv0.at[k, i]), s0s.at[0], r0.at[k, i], **to(core_peer)).wait_recv()

        def s0(self, c, first):
            def ready(k):
                if first:
                    @pl.when(c > 0)
                    def _():
                        for j in range(2):
                            big.s2_copy(k, j).wait_send()
                        big.s0_copy(k, first, 1).wait_send()
                else:
                    for j in range(2):
                        self.s0_copy(k, first, j).wait_send()

            self.pairs(c, c * D_STEPS + (0 if first else 6), ready, lambda k, i2: [], lambda k, j: k * 2 + j,
                       lambda k, j: self.s0_copy(k, first, j).start())

        def s1_copy(self, k, j):
            _, b2, _ = bits(k)
            i2 = 1 - b2 if j == 0 else b2
            return pltpu.make_async_remote_copy(
                self.whole(st.at[6 + k * 2 + j]), self.whole(rv1.at[k, i2]), s1s.at[k, j], r1.at[k, i2],
                **to(peer(dim(k, 0))))

        def r1_wait(self, k, i2):
            pltpu.make_async_remote_copy(
                self.whole(st.at[6]), self.whole(rv1.at[k, i2]), s1s.at[k, 0], r1.at[k, i2],
                **to(peer(dim(k, 0)))).wait_recv()

        def s1(self, c):
            def index(k, j):
                b1, b2, _ = bits(k)
                return (1 - b1) * 2 + (1 - b2 if j == 0 else b2)

            def ready(k):
                for j in range(2):
                    self.r0_wait(k, index(k, j))

                @pl.when(c > 0)
                def _():
                    big.f_wait(c - 1, k, True)
                    big.s1_copy(k, 1).wait_send()

            self.pairs(c, c * D_STEPS + 3, ready, lambda k, i2: [rv0.at[k, (1 - bits(k)[0]) * 2 + i2]],
                       lambda k, j: 6 + k * 2 + j, lambda k, j: self.s1_copy(k, j).start())

        def s2_copy(self, k, i):
            b3 = bits(k)[2]
            part = pl.ds(pl.multiple_of((1 - b3 if i == 0 else b3) * self.half, 16), self.half)
            return pltpu.make_async_remote_copy(
                st.at[k * 2, part], rv2.at[k, part], s2s.at[k, i], r2.at[k, i], **to(peer(dim(k, 1))))

        def s2(self, c):
            def body(k):
                b1, b2, _ = bits(k)
                i = b1 * 2 + 1 - b2
                step = c * D_STEPS + 9 + k
                d_copy(step).wait()
                self.r0_wait(k, i)
                self.r1_wait(k, 1 - b2)
                self.s0_copy(k, False, 0).wait_send()
                y = self.down(c, k, 1 - b2)
                for a in (rv0.at[k, i], rv1.at[k, 1 - b2]):
                    y = y + a[pl.ds(0, self.R)].astype(F32)
                st[k * 2, pl.ds(0, self.R)] = y.astype(BF16)
                raw[k, pl.ds(0, self.R)] = self.down(c, k, b2)
                for i in range(2):
                    self.s2_copy(k, i).start()
                d_start(step + 3)

            for k in range(3):
                body(k)

        def last(self, k, part, more):
            b1, b2, _ = bits(k)
            rows = pl.ds(pl.multiple_of(part * self.half, 16), self.half)
            y = raw[k, rows]
            for a in (rv0.at[k, b1 * 2 + b2], rv1.at[k, b2], rv2.at[k]):
                y = y + a[rows].astype(F32)
            if more:
                y = y + rv3[k, pl.ds(0, self.half)].astype(F32)
            st[6 + k * 2, pl.ds(0, self.half)] = y.astype(BF16)

        def s3_copy(self, k):
            n = pl.ds(0, self.half)
            return pltpu.make_async_remote_copy(
                st.at[6 + k * 2, n], rv3.at[k, n], s3s.at[k], r3.at[k], **to(peer(dim(k, 2))))

        def s3(self, c):
            def body(k):
                b1, b2, b3 = bits(k)
                self.r0_wait(k, b1 * 2 + b2)
                self.r1_wait(k, b2)
                self.s2_copy(k, 0).wait_recv()
                self.s1_copy(k, 0).wait_send()
                self.last(k, 1 - b3, False)
                self.s3_copy(k).start()

            loop(3, body)

        def place(self, c, k, i1, i2, part):
            row = pl.multiple_of(c * BIG + part * self.half, 16)
            return y_hbm.at[pl.ds(row, self.half), pl.ds(col(k, b0, i1, i2), CB)]

        def f_copies(self, c, k):
            b1, b2, b3 = bits(k)
            par = lax.rem(c, 2)
            src, dst = st.at[6 + k * 2, pl.ds(0, self.half)], self.place(c, k, b1, b2, b3)
            return [
                pltpu.make_async_remote_copy(src, dst, fs.at[k, 0], g3.at[par, k], **to(peer(dim(k, 2)))),
                pltpu.make_async_remote_copy(src, dst, fs.at[k, 1], g2.at[par, k, 0], **to(peer(dim(k, 1)))),
                pltpu.make_async_remote_copy(src, dst, fs.at[k, 2], g1.at[par, k, 0], **to(peer(dim(k, 0)))),
                pltpu.make_async_copy(src, dst, fl.at[k]),
            ]

        def f_wait(self, c, k, copies):
            for cp in self.f_copies(c, k)[:3]:
                cp.wait_send()
            if copies:
                self.f_copies(c, k)[3].wait()

        def fin(self, c):
            def body(k):
                _, _, b3 = bits(k)
                self.s2_copy(k, 1).wait_recv()
                self.s3_copy(k).wait_recv()
                self.s3_copy(k).wait_send()
                self.last(k, b3, True)
                copies = self.f_copies(c, k)
                copies[0].start()
                copies[3].start()

            loop(3, body)
            for i in (1, 2):
                loop(3, lambda k, i=i: self.f_copies(c, k)[i].start())

            @pl.when(c < nc - 1)
            def _():
                for i, dev in enumerate(everyone):
                    pl.semaphore_signal(credit.at[i], inc=1, **to(dev))

        def part_of_y(self, c, col0, width):
            return y_hbm.at[pl.ds(pl.multiple_of(c * BIG, 32), self.R), pl.ds(col0, width)]

        def a3_copies(self, c, k):
            b1, b2, b3 = bits(k)
            par = lax.rem(c, 2)
            p = self.place(c, k, b1, b2, 1 - b3)
            return [
                pltpu.make_async_remote_copy(p, p, a3s.at[k, 0], g2.at[par, k, 1], **to(peer(dim(k, 1)))),
                pltpu.make_async_remote_copy(p, p, a3s.at[k, 1], g1.at[par, k, 1], **to(peer(dim(k, 0)))),
            ]

        def a2_copies(self, c, k):
            b1, b2, b3 = bits(k)
            par = lax.rem(c, 2)
            block = self.part_of_y(c, col(k, b0, b1, 1 - b2), CB)
            pieces = [self.place(c, k, b1, 1 - b2, b3), self.place(c, k, b1, 1 - b2, 1 - b3)]
            q = self.part_of_y(c, col(k, b0, b1, 0), 2 * CB)
            return [
                pltpu.make_async_remote_copy(p, p, a2s.at[k, i], g1.at[par, k, 2 + i], **to(peer(dim(k, 0))))
                for i, p in enumerate(pieces if self is small else [block])
            ] + [pltpu.make_async_remote_copy(q, q, a2s.at[k, 2], g0.at[c, k, 0], **to(core_peer))]

        def a1_parts(self, c, k):
            b1, b2, _ = bits(k)
            if self is small:
                return [self.part_of_y(c, col(k, b0, 1 - b1, i2), CB) for i2 in (b2, 1 - b2)]
            return [self.part_of_y(c, col(k, b0, 1 - b1, 0), 2 * CB)]

        def a1_copies(self, c, k):
            return [pltpu.make_async_remote_copy(q, q, a1s.at[k, i], g0.at[c, k, 1 + i], **to(core_peer))
                    for i, q in enumerate(self.a1_parts(c, k))]

        def landed(self, sem, p):
            pltpu.make_async_remote_copy(p, p, a1s.at[0, 0], sem, **to(core_peer)).wait_recv()

        def sent(self, c, copies):
            def body(k):
                for cp in copies(c, k):
                    cp.wait_send()

            loop(3, body)

        def a3_wait(self, c):
            self.sent(c, self.a3_copies)

        def a2_wait(self, c):
            self.sent(c, self.a2_copies)

        def a1_wait(self, c):
            self.sent(c, self.a1_copies)

        def a3(self, c):
            pl.when(c > 0)(lambda: big.a3_wait(c - 1))

            def body(k):
                b1, b2, b3 = bits(k)
                self.landed(g3.at[lax.rem(c, 2), k], self.place(c, k, b1, b2, 1 - b3))
                for cp in self.a3_copies(c, k):
                    cp.start()

            loop(3, body)

        def a2(self, c):
            pl.when(c > 0)(lambda: big.a2_wait(c - 1))

            def piece(k, i):
                b1, b2, b3 = bits(k)
                self.landed(g2.at[lax.rem(c, 2), k, i], self.place(c, k, b1, 1 - b2, b3 if i == 0 else 1 - b3))

            def first(k):
                self.f_copies(c, k)[3].wait()
                piece(k, 0)
                self.a2_copies(c, k)[0].start()

            def body(k):
                if self is not small:
                    piece(k, 0)
                piece(k, 1)
                for cp in self.a2_copies(c, k)[1 if self is small else 0 :]:
                    cp.start()

            if self is small:
                loop(3, first)
            loop(3, body)

        def a1(self, c):
            pl.when(c > 0)(lambda: big.a1_wait(c - 1))

            def near(k):
                b1, b2, b3 = bits(k)
                for i, part in enumerate((b3, 1 - b3)):
                    self.landed(g1.at[lax.rem(c, 2), k, i], self.place(c, k, 1 - b1, b2, part))

            def far(k):
                b1, b2, b3 = bits(k)
                if self is small:
                    for i, part in enumerate((b3, 1 - b3)):
                        self.landed(g1.at[lax.rem(c, 2), k, 2 + i], self.place(c, k, 1 - b1, 1 - b2, part))
                else:
                    self.landed(g1.at[lax.rem(c, 2), k, 2], self.part_of_y(c, col(k, b0, 1 - b1, 1 - b2), CB))

            def first(k):
                near(k)
                self.a1_copies(c, k)[0].start()

            def body(k):
                if self is not small:
                    near(k)
                far(k)
                self.a1_copies(c, k)[-1].start()

            if self is small:
                loop(3, first)
            loop(3, body)

        def a0_wait(self, c):
            def body(k):
                b1, _, _ = bits(k)
                self.landed(g0.at[c, k, 0], self.part_of_y(c, col(k, 1 - b0, b1, 0), 2 * CB))
                if self is small:
                    _, b2, _ = bits(k)
                    for i, i2 in enumerate((b2, 1 - b2)):
                        self.landed(g0.at[c, k, 1 + i], self.part_of_y(c, col(k, 1 - b0, 1 - b1, i2), CB))
                else:
                    self.landed(g0.at[c, k, 1], self.part_of_y(c, col(k, 1 - b0, 1 - b1, 0), 2 * CB))

            loop(3, body)

        def early(self, c):
            self.gu_epilogue(c, nt - 1)

            @pl.when(c > 0)
            def _():
                for i in range(4):
                    pl.semaphore_wait(credit.at[i], 1)

            self.s0(c, True)
            self.s1(c)
            either(c + 1, lambda a: a.x_copy(c + 1, 1).start(priority=1))
            self.s0(c, False)

    big, small = Chunk(BIG), Chunk(rows - nb * BIG)

    def either(c, act):
        pl.when((c >= 0) & (c < nb))(lambda: act(big))
        pl.when(c == nb)(lambda: act(small))

    for i in range(PACKETS):
        for cp in w_copies(0, i, i):
            cp.start()
        big.x_copy(0, i).start()

    barrier = pltpu.get_barrier_semaphore()
    everyone = [peer(0), peer(1), peer(2), core_peer]
    for dev in everyone:
        pl.semaphore_signal(barrier, inc=1, **to(dev))
    pl.semaphore_wait(barrier, 4)

    rooms = kept_parts(depth, y_hbm, wbuf, xv)

    def keep(act):
        base = 0
        for count, part in rooms:
            loop(count, lambda i, base=base, part=part: act(pltpu.make_async_copy(*part(i), k_sem.at[base + i])))
            base += count

    def chunk(c):
        def tile(n):
            for i in range(PACKETS):
                either(c, lambda a: a.gate_up(c, n, i))
                if i == 0:
                    pl.when((c == 0) & (n >= 3) & (n < 6))(lambda: d_copy(n - 3).start())

                for slot in sorted({slot for slot, _, _ in SLOTS if slot % PACKETS == i}):
                    @pl.when(n == slot // PACKETS)
                    def _(slot=slot):
                        for at, act, lag in SLOTS:
                            if at == slot:
                                either(c - lag, lambda a, act=act, lag=lag: getattr(a, act)(c - lag))
                        if slot == 1:
                            @pl.when(c == nc)
                            def _():
                                loop(nc - 2, lambda i: big.a0_wait(i))
                                keep(lambda cp: cp.start())

        loop(nt, tile)
        either(c, lambda a: a.early(c))

    loop(nc + 2, chunk)

    last = nc - 1
    def drain(k):
        small.s0_copy(k, False, 1).wait_send()
        small.s1_copy(k, 1).wait_send()
        for j in range(2):
            small.s2_copy(k, j).wait_send()
        small.f_wait(last, k, False)

    loop(3, drain)
    small.a3_wait(last)
    small.a2_wait(last)
    small.a1_wait(last)
    big.a0_wait(nc - 2)
    small.a0_wait(nc - 1)
    keep(lambda cp: cp.wait())


def block(x, wg, wu, wd):
    rows, depth = x.shape
    units = wg.shape[1]
    nc = rows // BIG + 1
    kb = depth // PACKETS
    dma, vmem = pltpu.SemaphoreType.DMA, pltpu.VMEM
    y, wbuf, xv = pl.pallas_call(
        kernel,
        name="mlp",
        out_shape=[
            jax.ShapeDtypeStruct((rows, depth), BF16),
            vmem((W_SLOTS, kb, 2 * GN), BF16),
            vmem((PACKETS, BIG, kb), BF16),
        ],
        in_specs=[pl.BlockSpec(memory_space=pl.ANY)] * 4,
        out_specs=[pl.BlockSpec(memory_space=pl.ANY)] + [pl.BlockSpec(memory_space=pltpu.VMEM)] * 2,
        scratch_shapes=[
            vmem((BIG, 2 * GN), F32),
            vmem((2, BIG, units), BF16),
            vmem((3, units, 2 * CB), BF16),
            vmem((3, BIG, CB), F32),
            vmem((3, 4, BIG, CB), BF16),
            vmem((3, 2, BIG, CB), BF16),
            vmem((3, BIG, CB), BF16),
            vmem((3, BIG // 2, CB), BF16),
            vmem((12, BIG, CB), BF16),
            dma((PACKETS,)), dma((W_SLOTS, 2)), dma((3,)),
            dma((6,)), dma((3, 2)), dma((3, 2)), dma((3,)), dma((3, 3)), dma((3,)),
            dma((3, 2)), dma((3, 3)), dma((3, 2)),
            dma((3, 4)), dma((3, 2)), dma((3, 2)), dma((3,)),
            dma((2, 3)), dma((2, 3, 2)), dma((2, 3, 4)), dma((nc, 3, 3)),
            dma((depth // CB + PACKETS,)),
            pltpu.SemaphoreType.REGULAR((4,)),
        ],
        compiler_params=pltpu.CompilerParams(
            collective_id=0, has_side_effects=True, vmem_limit_bytes=75 * 2**19
        ),
    )(x, wg, wu, wd)

    return pl.pallas_call(
        put,
        name="put",
        out_shape=jax.ShapeDtypeStruct((rows, depth), BF16),
        in_specs=[pl.BlockSpec(memory_space=pl.ANY)] + [pl.BlockSpec(memory_space=pltpu.VMEM)] * 2,
        out_specs=pl.BlockSpec(memory_space=pl.ANY),
        scratch_shapes=[
            vmem((STRIPS, STRIP, depth), BF16),
            dma((depth // CB + PACKETS,)),
            dma((STRIPS, 2)),
        ],
        compiler_params=pltpu.CompilerParams(vmem_limit_bytes=7 * 2**20),
    )(y, wbuf, xv)


def put(y_hbm, wbuf, xv, o_hbm, buf, k_sem, sem):
    rows, depth = o_hbm.shape
    first = sum(kept(depth))
    count = (rows - first) // STRIP

    def strip(i):
        part, slot = pl.ds(pl.multiple_of(first + i * STRIP, STRIP), STRIP), lax.rem(i, STRIPS)
        return (pltpu.make_async_copy(y_hbm.at[part], buf.at[slot], sem.at[slot, 0]),
                pltpu.make_async_copy(buf.at[slot], o_hbm.at[part], sem.at[slot, 1]))

    def keep(act):
        base = 0
        for n, part in kept_parts(depth, o_hbm, wbuf, xv):
            def one(i, _, base=base, part=part):
                dst, src = part(i)
                act(pltpu.make_async_copy(src, dst, k_sem.at[base + i]))
                return 0

            lax.fori_loop(0, n, one, 0)
            base += n

    for i in range(AHEAD):
        strip(i)[0].start()
    keep(lambda cp: cp.start())

    def step(i, _):
        strip(i)[0].wait()
        strip(i)[1].start()
        j = i + AHEAD

        @pl.when(j < count)
        def _():
            pl.when(j >= STRIPS)(lambda: strip(j - STRIPS)[1].wait())
            strip(j)[0].start()

        return 0

    lax.fori_loop(0, count, step, 0)
    keep(lambda cp: cp.wait())
    for i in range(count - STRIPS, count):
        strip(i)[1].wait()


def solution(mesh):
    return jax.shard_map(
        block,
        mesh=mesh,
        in_specs=(P("dp", None), P(None, "tp"), P(None, "tp"), P("tp", None)),
        out_specs=P("dp", None),
        check_vma=False,
    )
```
